256 devices in a mesh: space: 32 (over z, y_hi, core), tm: 8 (over x, y_lo).
Axes of the slice: x: 4, y: 4 (y_hi: 2, y_lo: 2; y = y_hi * 2 + y_lo), z: 8, core: 2. Of those that a mesh axis runs over, the one named last changes fastest.
Arguments:
- solutions: bfloat16 [8, 12, 16384, 128], P('tm', None, 'space'), may hold values from -6 to 6
- noise: int32 [8, 64, 12, 16384], P('tm', None, None, 'space'), may hold values from 0 to 3
- momenta: int32 [27, 3], replicated, may hold values from -2 to 2
- pairs: int32 [64, 2], P('tm'), may hold values from 0 to 7
Outputs:
- mesons: float32 [8, 2, 27, 64, 64], P('tm', None, None, 'space')
- correlators: float32 [64, 2, 27], P('tm')
The draws below stay inside these ranges and needn't reach their ends.
All inputs are finite; a program needn't handle non-finite values.
Results may differ from the reference program's by a relative error of at most 0.002.
Values sent between devices are 32-bit elements; how exact they have to be, the bound alone decides.
No kernel may reach another device: no remote copies, remote signals or barrier semaphores. Data moves between devices by JAX's collectives and lax.ppermute only.
A program may use at most 64 MiB of HBM per device.

```python
import math
import jax
import jax.numpy as jnp
from jax import lax

NVEC = 64
SPINCOL = 12
MOMS = 27
EXTENT = 48
SITES = 16384
TSL = 8
NPAIRS = 64


def plant(drawn, rng, least, top_value):
    place = [jax.random.randint(jax.random.fold_in(rng, axis), (), 0, length) for axis, length in enumerate(drawn.shape)]
    main_axis = drawn.shape.index(max(drawn.shape))
    next_to = place[:main_axis] + [(place[main_axis] + 1) % drawn.shape[main_axis]] + place[main_axis + 1:]
    return drawn.at[tuple(place)].set(least).at[tuple(next_to)].set(top_value)


def level_of(key, extent, cuts, least, top_value):
    gain, own = 1.0, jax.random.fold_in(key, 6)
    for dim, parts in cuts:
        draws = jnp.exp(jax.random.uniform(jax.random.fold_in(own, dim), (parts,), jnp.float32, least / len(cuts), top_value / len(cuts)))
        gain = gain * jnp.repeat(draws, extent[dim] // parts).reshape([-1 if axis == dim else 1 for axis in range(len(extent))])
    return gain


def bell_draw(key, dims, scale, reach, split=(), held_as=jnp.bfloat16):
    result = jax.random.normal(key, dims, jnp.float32) * scale
    if len(split) > 0:
        result = level_of(key, dims, split, -0.22, 0.18) * result
    return jnp.clip(result, min=-reach, max=reach).astype(held_as)


def setup_inputs(seed: int = 0) -> dict:
    splits = jax.random.split(jax.random.key(seed), 5)
    return {
        "solutions": bell_draw(splits[0], (TSL, SPINCOL, SITES, 2 * NVEC), 1.0, 6.0, ((0, 8), (2, 32))),
        "noise": plant(jax.random.randint(splits[1], (TSL, NVEC, SPINCOL, SITES), 0, 4), jax.random.fold_in(splits[1], 1), 0, 3).astype(jnp.int32),
        "momenta": plant(jax.random.randint(splits[2], (MOMS, 3), -2, 3), jax.random.fold_in(splits[2], 1), -2, 2).astype(jnp.int32),
        "pairs": plant(jax.random.randint(splits[3], (NPAIRS, 2), 0, TSL), jax.random.fold_in(splits[3], 1), 0, TSL - 1).astype(jnp.int32),
    }


def phase_weights(noise_block, momenta, coords):
    qdotx = momenta[:, 0:1] * coords[0][None, :] + momenta[:, 1:2] * coords[1][None, :] + momenta[:, 2:3] * coords[2][None, :]
    index = (EXTENT // 4 * noise_block[None, :, :, :] + qdotx[:, None, None, :]) % EXTENT
    angle = index.astype(jnp.float32) * jnp.float32(2.0 * math.pi / EXTENT)
    rows = momenta.shape[0] * noise_block.shape[0]
    cols = noise_block.shape[1] * noise_block.shape[2]
    weight_re = jnp.cos(angle).astype(jnp.bfloat16).reshape(rows, cols)
    weight_im = (-jnp.sin(angle)).astype(jnp.bfloat16).reshape(rows, cols)
    return (weight_re, weight_im)

def site_coords(first, count):
    glob = first + jnp.arange(count, dtype=jnp.int32)
    return (glob % EXTENT, glob // EXTENT % EXTENT, glob // (EXTENT * EXTENT))

def slice_field(vectors, sources, momenta):
    block = min(1024, SITES)
    nblocks = SITES // block

    def one_block(step, total):
        first = (step * block).astype(jnp.int32)
        noise_block = lax.dynamic_slice_in_dim(sources, first, block, 2)
        vec_block = lax.dynamic_slice_in_dim(vectors, first, block, 1)
        weight_re, weight_im = phase_weights(noise_block, momenta, site_coords(first, block))
        stacked = vec_block.reshape(SPINCOL * block, 2 * NVEC)
        left = jnp.dot(weight_re, stacked, preferred_element_type=jnp.float32)
        right = jnp.dot(weight_im, stacked, preferred_element_type=jnp.float32)
        real_part = left[:, :NVEC] - right[:, NVEC:]
        imag_part = left[:, NVEC:] + right[:, :NVEC]
        return total + jnp.stack([real_part, imag_part], 0)
    start = jnp.zeros((2, MOMS * NVEC, NVEC), jnp.float32)
    total = lax.fori_loop(0, nblocks, one_block, start)
    return total.reshape(2, MOMS, NVEC, NVEC)

def reference(solutions, noise, momenta, pairs):
    scale = 1.0 / math.sqrt(SPINCOL * SITES)
    fields = [slice_field(solutions[t], noise[t], momenta) * scale for t in range(TSL)]
    mesons = jnp.stack(fields, 0)
    sink = mesons[pairs[:, 1]]
    source = mesons[pairs[:, 0]]
    real_part = lax.optimization_barrier(jnp.sum(sink[:, 0] * source[:, 0] + sink[:, 1] * source[:, 1], axis=(2, 3)))
    imag_part = lax.optimization_barrier(jnp.sum(sink[:, 1] * source[:, 0] - sink[:, 0] * source[:, 1], axis=(2, 3)))
    correlators = jnp.stack([real_part, imag_part], 1) / NVEC
    return (mesons, correlators)
```

```python
import functools
import math

import jax
import jax.numpy as jnp
import numpy as np
from jax import lax
from jax.experimental import pallas as pl
from jax.experimental.pallas import tpu as pltpu
from jax.sharding import Mesh
from jax.sharding import PartitionSpec as P

EXTENT = 48
LANES = 128
SITE_BLOCK = 64
QX = 5
ZY = 16
GROUP = 28
CHUNK = 2 * GROUP


def trig_table():
    angle = (np.arange(LANES) % EXTENT) * (2.0 * np.pi / EXTENT)
    rows = np.stack([np.cos(angle), np.sin(angle)]).astype(np.float32)
    return np.repeat(rows, 8, axis=0)


def lane_iota(rows):
    return lax.broadcasted_iota(jnp.int32, (rows, LANES), 1)


def looked_up(table, index):
    return jnp.take_along_axis(table, index, axis=1)


def field_kernel(where_ref, mom_ref, table_ref, noise_ref, vec_ref, peer_ref, own_ref, phase_re, phase_im, w_ref, v_ref, d_ref, m_ref):
    nmom = mom_ref.shape[0]
    step = pl.program_id(0)
    offset = where_ref[0]
    core = where_ref[1]
    spincol = noise_ref.shape[0]
    half = spincol * SITE_BLOCK
    cos_table = table_ref[0:8, :]
    sin_table = table_ref[8:16, :]
    lane8 = lane_iota(8)
    low8 = lane8 < SITE_BLOCK
    low64 = lane_iota(64) < SITE_BLOCK

    @pl.when(step == 0)
    def _():
        first = offset + SITE_BLOCK * lax.broadcasted_iota(jnp.int32, (8, LANES), 0)
        line = first // EXTENT + jnp.where(low8, 0, 1)
        y, z = (lax.rem(line, EXTENT), lax.div(line, EXTENT))

        def per_momentum(q, carry):
            index = mom_ref[q, 1] * y + mom_ref[q, 2] * z
            index = jnp.where(index < 0, index + 3 * EXTENT, index)
            index = jnp.where(index >= 2 * EXTENT, index - 2 * EXTENT, index)
            phase_re[q] = looked_up(cos_table, index)
            phase_im[q] = -looked_up(sin_table, index)
            return carry

        lax.fori_loop(0, nmom, per_momentum, 0)
        m_ref[...] = jnp.zeros_like(m_ref)
        zero = jnp.zeros((ZY, LANES), jnp.float32)
        for out in (peer_ref, own_ref):
            for b in range(2):
                out[pl.ds(b * GROUP + GROUP - 1, ZY, stride=CHUNK), :] = zero

    bounds, waves = ([], [])
    for g in range(2):
        first = offset + step * 2 * SITE_BLOCK + g * SITE_BLOCK
        into = lax.rem(first, EXTENT)
        bounds.append(EXTENT - into)
        x = into + (lane8 & (SITE_BLOCK - 1))
        x = jnp.where(x >= EXTENT, x - EXTENT, x)
        x2 = 2 * x
        x2 = jnp.where(x2 >= EXTENT, x2 - EXTENT, x2)
        waves.append([looked_up(t, i)[0:1, :].astype(jnp.bfloat16) for i in (x, x2) for t in (cos_table, sin_table)])

    one = jnp.bfloat16(1)
    two = jnp.bfloat16(2)
    for pair in range(spincol // 2):
        rows = []
        for a in (2 * pair, 2 * pair + 1):
            parts = [noise_ref[a, pl.ds(c * 2 + b, ZY, stride=4), :] for c in (1 - core, core) for b in range(2)]
            rows.append(jnp.concatenate(parts, axis=0))
        turned = [pltpu.roll(r, SITE_BLOCK, 1) for r in rows]
        blocks = (jnp.where(low64, rows[0], turned[1]), jnp.where(low64, turned[0], rows[1]))
        cols = pl.ds(pair * LANES, LANES)
        cols_im = pl.ds(half + pair * LANES, LANES)
        for g in range(2):
            turns = blocks[g].astype(jnp.float32).astype(jnp.bfloat16)
            er = jnp.abs(turns - two) - one
            ei = one - jnp.abs(turns - one)
            w_ref[g, 2 * 64 : 3 * 64, cols] = er
            w_ref[g, 2 * 64 : 3 * 64, cols_im] = -ei
            for k in (1, 2):
                c, s = waves[g][2 * (k - 1) : 2 * k]
                erc, eis, ers, eic = (er * c, ei * s, er * s, ei * c)
                up, down = ((2 + k) * 64, (2 - k) * 64)
                w_ref[g, up : up + 64, cols] = erc - eis
                w_ref[g, up : up + 64, cols_im] = -(ers + eic)
                w_ref[g, down : down + 64, cols] = erc + eis
                w_ref[g, down : down + 64, cols_im] = ers - eic

    site = lax.broadcasted_iota(jnp.int32, (SITE_BLOCK, LANES), 0)
    for g in range(2):
        mask = jnp.where((site < bounds[g]) == low64, 1.0, 0.0).astype(jnp.bfloat16)
        for a in range(spincol):
            v = vec_ref[a, g * SITE_BLOCK : (g + 1) * SITE_BLOCK, :]
            re = jnp.concatenate([v[:, :SITE_BLOCK], v[:, :SITE_BLOCK]], axis=1) * mask
            im = jnp.concatenate([v[:, SITE_BLOCK:], v[:, SITE_BLOCK:]], axis=1) * mask
            k0, k1 = (a * SITE_BLOCK, half + a * SITE_BLOCK)
            v_ref[g, k0 : k0 + SITE_BLOCK, 0:LANES] = re
            v_ref[g, k0 : k0 + SITE_BLOCK, LANES:] = im
            v_ref[g, k1 : k1 + SITE_BLOCK, 0:LANES] = -im
            v_ref[g, k1 : k1 + SITE_BLOCK, LANES:] = re

    for g in range(2):
        d_ref[g] = jnp.dot(w_ref[g], v_ref[g], preferred_element_type=jnp.float32)

    def add_momentum(q, carry):
        row = pl.multiple_of((mom_ref[q, 0] + 2) * 64, 64)
        re, im = (m_ref[q, 0], m_ref[q, 1])
        for g in range(2):
            fr = phase_re[q, pl.ds(step * 2 + g, 1), :]
            fi = phase_im[q, pl.ds(step * 2 + g, 1), :]
            dr = d_ref[g, pl.ds(row, 64), 0:LANES]
            di = d_ref[g, pl.ds(row, 64), LANES:]
            re = re + (fr * dr - fi * di)
            im = im + (fr * di + fi * dr)
        m_ref[q, 0] = re
        m_ref[q, 1] = im
        return carry

    lax.fori_loop(0, nmom, add_momentum, 0)

    @pl.when(step == pl.num_programs(0) - 1)
    def _():
        def finish(q, carry):
            re, im = (m_ref[q, 0], m_ref[q, 1])
            kept = jnp.where(low64, re, im)
            moved = pltpu.roll(jnp.where(low64, im, re), SITE_BLOCK, 1)
            total = kept + moved
            for n, out in enumerate((peer_ref, own_ref)):
                for b in range(2):
                    r = n * 32 + b * ZY
                    out[pl.ds(b * GROUP + q, ZY, stride=CHUNK), :] = total[r : r + ZY]
            return carry

        lax.fori_loop(0, nmom, finish, 0)


def partial_fields(where, momenta, noise, vectors):
    nmom = momenta.shape[0]
    spincol, nvec, sites = noise.shape
    smem = pl.BlockSpec(memory_space=pltpu.SMEM)
    out = jax.ShapeDtypeStruct((ZY * CHUNK, LANES), jnp.float32)
    out_spec = pl.BlockSpec((ZY * CHUNK, LANES), lambda s: (0, 0))
    depth = 2 * spincol * SITE_BLOCK
    return pl.pallas_call(
        field_kernel,
        grid=(sites // LANES,),
        in_specs=[
            smem,
            smem,
            pl.BlockSpec((16, LANES), lambda s: (0, 0)),
            pl.BlockSpec((spincol, nvec, LANES), lambda s: (0, 0, s)),
            pl.BlockSpec((spincol, LANES, LANES), lambda s: (0, s, 0)),
        ],
        out_specs=[out_spec, out_spec],
        out_shape=[out, out],
        scratch_shapes=[
            pltpu.VMEM((nmom, 8, LANES), jnp.float32),
            pltpu.VMEM((nmom, 8, LANES), jnp.float32),
            pltpu.VMEM((2, QX * nvec, depth), jnp.bfloat16),
            pltpu.VMEM((2, depth, 2 * LANES), jnp.bfloat16),
            pltpu.VMEM((2, QX * nvec, 2 * LANES), jnp.float32),
            pltpu.VMEM((nmom, 2, nvec, LANES), jnp.float32),
        ],
        name="fields",
    )(where, momenta, jnp.asarray(trig_table()), noise, vectors)


def mesons_kernel(scale, part_ref, copies_ref, out_ref, row_ref):
    total = part_ref[0]
    for n in range(1, part_ref.shape[0]):
        total = total + part_ref[n]
    total = total * scale
    for n in range(copies_ref.shape[0]):
        copies_ref[n] = total
    row_ref[...] = total
    for q in range(out_ref.shape[2]):
        for b in range(2):
            r = b * GROUP + q
            for c in range(2):
                out_ref[0, c, q, b : b + 1, :] = row_ref[r : r + 1, c * 64 : (c + 1) * 64]


def summed_mesons(parts, scale, copies, nmom):
    return pl.pallas_call(
        functools.partial(mesons_kernel, scale),
        out_shape=[
            jax.ShapeDtypeStruct((copies, CHUNK, LANES), jnp.float32),
            jax.ShapeDtypeStruct((1, 2, nmom, 2, 64), jnp.float32),
        ],
        scratch_shapes=[pltpu.VMEM((CHUNK, LANES), jnp.float32)],
        name="mesons",
    )(parts)


def traces_kernel(pairs_ref, fields_ref, out_ref):
    lane = lane_iota(CHUNK)
    sign = jnp.where(lane < 64, -1.0, 1.0)
    re = jnp.zeros((LANES, LANES), jnp.float32)
    re = jnp.zeros((CHUNK, LANES), jnp.float32)
    im = re
    for k in range(pairs_ref.shape[0]):
        source = fields_ref[pairs_ref[k, 0]]
        sink = fields_ref[pairs_ref[k, 1]]
        swapped = pltpu.roll(source, 64, 1) * sign
        re = jnp.where(lane == k, jnp.sum(sink * source, axis=1, keepdims=True), re)
        im = jnp.where(lane == k, jnp.sum(sink * swapped, axis=1, keepdims=True), im)
    pad = jnp.zeros((64 - CHUNK, LANES), jnp.float32)
    both = jnp.concatenate([re, pad, im, pad], axis=0)
    out_ref[...] = both.T[0:8, :]


def partial_traces(pairs, fields):
    smem = pl.BlockSpec(memory_space=pltpu.SMEM)
    return pl.pallas_call(
        traces_kernel,
        in_specs=[smem, pl.BlockSpec(memory_space=pltpu.VMEM)],
        out_shape=jax.ShapeDtypeStruct((8, LANES), jnp.float32),
        name="traces",
    )(pairs, fields)


def correlators_kernel(factor, part_ref, out_ref):
    total = part_ref[0]
    for n in range(1, part_ref.shape[0]):
        total = total + part_ref[n]
    total = total * factor
    nmom = out_ref.shape[2]
    total = total + pltpu.roll(total, LANES - GROUP, 1)
    moved = pltpu.roll(total, 64, 1)
    for k in range(out_ref.shape[0]):
        out_ref[k, 0:1, :] = total[k : k + 1, 0:nmom]
        out_ref[k, 1:2, :] = moved[k : k + 1, 0:nmom]


def summed_traces(parts, factor, npairs, nmom):
    return pl.pallas_call(
        functools.partial(correlators_kernel, factor),
        out_shape=jax.ShapeDtypeStruct((npairs, 2, nmom), jnp.float32),
        name="correlators",
    )(parts)


def exchange(array, axis):
    return lax.all_to_all(array, axis, split_axis=0, concat_axis=0, tiled=True)


def local(solutions, noise, momenta, pairs):
    spincol, sites, width = solutions.shape[1:]
    nmom = momenta.shape[0]
    core = lax.axis_index("core")
    place = lax.axis_index(("z", "yh", "core"))
    where = jnp.stack([place * sites, core]).astype(jnp.int32)
    peer, own = partial_fields(where, momenta, jnp.swapaxes(noise[0], 0, 1), solutions[0])
    arrived = lax.ppermute(peer, "core", [(0, 1), (1, 0)])
    chunks = (own + arrived).reshape(ZY, CHUNK, LANES)
    scale = 1.0 / math.sqrt(spincol * sites * 2 * ZY)
    copies, mesons = summed_mesons(exchange(chunks, ("z", "yh")), scale, lax.axis_size("tm"), nmom)
    traces = partial_traces(pairs, exchange(copies, "tm"))
    traces = traces + lax.ppermute(traces, "core", [(0, 1), (1, 0)])
    spread = jnp.broadcast_to(traces, (ZY, *traces.shape))
    correlators = summed_traces(exchange(spread, ("z", "yh")), 1.0 / 64, pairs.shape[0], nmom)
    return (mesons, correlators)


def solution(mesh):
    split = Mesh(mesh.devices.reshape(8, 2, 2, 8), ("z", "yh", "core", "tm"))
    space = ("z", "yh", "core")
    in_specs = (P("tm", None, space, None), P("tm", None, None, space), P(), P("tm", None))
    out_specs = (P("tm", None, None, space, None), P("tm", None, None))
    return jax.shard_map(local, mesh=split, in_specs=in_specs, out_specs=out_specs, check_vma=False)
```

```python
import functools
import math

import jax
import jax.numpy as jnp
import numpy as np
from jax import lax
from jax.experimental import pallas as pl
from jax.experimental.pallas import tpu as pltpu
from jax.sharding import Mesh
from jax.sharding import PartitionSpec as P

EXTENT = 48
LANES = 128
SITE_BLOCK = 64
QX = 5
ZY = 16
GROUP = 28
CHUNK = 2 * GROUP


def grant(mebibytes):
    return pltpu.CompilerParams(vmem_limit_bytes=mebibytes << 20)


def trig_table():
    angle = (np.arange(LANES) % EXTENT) * (2.0 * np.pi / EXTENT)
    rows = np.stack([np.cos(angle), np.sin(angle)]).astype(np.float32)
    return np.repeat(rows, 8, axis=0)


def lane_iota(rows):
    return lax.broadcasted_iota(jnp.int32, (rows, LANES), 1)


def looked_up(table, index):
    return jnp.take_along_axis(table, index, axis=1)


def field_kernel(offset_ref, core_ref, mom_ref, table_ref, noise_ref, vec_ref, peer_ref, own_ref, phase_re, phase_im, w_ref, v_ref, d_ref, m_ref):
    nmom = mom_ref.shape[1]
    step = pl.program_id(0)
    offset = offset_ref[0]
    core = core_ref[0]
    spincol = noise_ref.shape[0]
    half = spincol * SITE_BLOCK
    cos_table = table_ref[0:8, :]
    sin_table = table_ref[8:16, :]
    lane8 = lane_iota(8)
    low8 = lane8 < SITE_BLOCK
    low64 = lane_iota(64) < SITE_BLOCK

    @pl.when(step == 0)
    def _():
        first = offset + SITE_BLOCK * lax.broadcasted_iota(jnp.int32, (8, LANES), 0)
        line = first // EXTENT + jnp.where(low8, 0, 1)
        y, z = (lax.rem(line, EXTENT), lax.div(line, EXTENT))

        for q in range(nmom):
            index = mom_ref[1, q] * y + mom_ref[2, q] * z
            index = jnp.where(index < 0, index + 3 * EXTENT, index)
            index = jnp.where(index >= 2 * EXTENT, index - 2 * EXTENT, index)
            phase_re[q] = looked_up(cos_table, index)
            phase_im[q] = -looked_up(sin_table, index)
        m_ref[...] = jnp.zeros_like(m_ref)
        zero = jnp.zeros((ZY, LANES), jnp.float32)
        for out in (peer_ref, own_ref):
            for b in range(2):
                out[pl.ds(b * GROUP + GROUP - 1, ZY, stride=CHUNK), :] = zero

    bounds, waves = ([], [])
    for g in range(2):
        first = offset + step * 2 * SITE_BLOCK + g * SITE_BLOCK
        into = lax.rem(first, EXTENT)
        bounds.append(EXTENT - into)
        x = into + (lane8 & (SITE_BLOCK - 1))
        x = jnp.where(x >= EXTENT, x - EXTENT, x)
        x2 = 2 * x
        x2 = jnp.where(x2 >= EXTENT, x2 - EXTENT, x2)
        waves.append([looked_up(t, i)[0:1, :].astype(jnp.bfloat16) for i in (x, x2) for t in (cos_table, sin_table)])

    one = jnp.bfloat16(1)
    two = jnp.bfloat16(2)
    for pair in range(spincol // 2):
        rows = []
        for a in (2 * pair, 2 * pair + 1):
            parts = [noise_ref[a, pl.ds(c * 2 + b, ZY, stride=4), :] for c in (1 - core, core) for b in range(2)]
            rows.append(jnp.concatenate(parts, axis=0))
        turned = [pltpu.roll(r, SITE_BLOCK, 1) for r in rows]
        blocks = (jnp.where(low64, rows[0], turned[1]), jnp.where(low64, turned[0], rows[1]))
        cols, cols_im = (pair, spincol // 2 + pair)
        for g in range(2):
            turns = blocks[g].astype(jnp.float32).astype(jnp.bfloat16)
            er = jnp.abs(turns - two) - one
            ei = one - jnp.abs(turns - one)
            w_ref[g, cols, 2 * 64 : 3 * 64] = er
            w_ref[g, cols_im, 2 * 64 : 3 * 64] = -ei
            for k in (1, 2):
                c, s = waves[g][2 * (k - 1) : 2 * k]
                erc, eis, ers, eic = (er * c, ei * s, er * s, ei * c)
                up, down = ((2 + k) * 64, (2 - k) * 64)
                w_ref[g, cols, up : up + 64] = erc - eis
                w_ref[g, cols_im, up : up + 64] = -(ers + eic)
                w_ref[g, cols, down : down + 64] = erc + eis
                w_ref[g, cols_im, down : down + 64] = ers - eic

    site = lax.broadcasted_iota(jnp.int32, (SITE_BLOCK, LANES), 0)
    for g in range(2):
        mask = jnp.where((site < bounds[g]) == low64, 1.0, 0.0).astype(jnp.bfloat16)
        for a in range(spincol):
            v = vec_ref[a, g * SITE_BLOCK : (g + 1) * SITE_BLOCK, :]
            turned = pltpu.roll(v, SITE_BLOCK, 1)
            re = jnp.where(low64, v, turned) * mask
            im = jnp.where(low64, turned, v) * mask
            k0, k1 = (a * SITE_BLOCK, half + a * SITE_BLOCK)
            v_ref[g, 0, k0 : k0 + SITE_BLOCK, :] = re
            v_ref[g, 1, k0 : k0 + SITE_BLOCK, :] = im
            v_ref[g, 0, k1 : k1 + SITE_BLOCK, :] = -im
            v_ref[g, 1, k1 : k1 + SITE_BLOCK, :] = re

    for g in range(2):
        left = jnp.concatenate([w_ref[g, n] for n in range(spincol)], axis=1)
        right = jnp.concatenate([v_ref[g, 0], v_ref[g, 1]], axis=1)
        d_ref[g] = jnp.dot(left, right, preferred_element_type=jnp.float32)

    def add_momentum(q, carry):
        row = pl.multiple_of((mom_ref[0, q] + 2) * 64, 64)
        re, im = (m_ref[q, 0], m_ref[q, 1])
        for g in range(2):
            fr = phase_re[q, pl.ds(step * 2 + g, 1), :]
            fi = phase_im[q, pl.ds(step * 2 + g, 1), :]
            dr = d_ref[g, pl.ds(row, 64), 0:LANES]
            di = d_ref[g, pl.ds(row, 64), LANES:]
            re = re + (fr * dr - fi * di)
            im = im + (fr * di + fi * dr)
        m_ref[q, 0] = re
        m_ref[q, 1] = im
        return carry

    lax.fori_loop(0, nmom, add_momentum, 0)

    @pl.when(step == pl.num_programs(0) - 1)
    def _():
        for q in range(nmom):
            re, im = (m_ref[q, 0], m_ref[q, 1])
            kept = jnp.where(low64, re, im)
            moved = pltpu.roll(jnp.where(low64, im, re), SITE_BLOCK, 1)
            total = kept + moved
            for n, out in enumerate((peer_ref, own_ref)):
                for b in range(2):
                    r = n * 32 + b * ZY
                    out[pl.ds(b * GROUP + q, ZY, stride=CHUNK), :] = total[r : r + ZY]


def partial_fields(offset, core, momenta, noise, vectors):
    nmom = momenta.shape[1]
    spincol, nvec, sites = noise.shape
    smem = pl.BlockSpec(memory_space=pltpu.SMEM)
    out = jax.ShapeDtypeStruct((ZY * CHUNK, LANES), jnp.float32)
    out_spec = pl.BlockSpec((ZY * CHUNK, LANES), lambda s: (0, 0))
    depth = 2 * spincol * SITE_BLOCK
    return pl.pallas_call(
        field_kernel,
        grid=(sites // LANES,),
        in_specs=[
            smem,
            smem,
            smem,
            pl.BlockSpec((16, LANES), lambda s: (0, 0)),
            pl.BlockSpec((spincol, nvec, LANES), lambda s: (0, 0, s)),
            pl.BlockSpec((spincol, LANES, LANES), lambda s: (0, s, 0)),
        ],
        out_specs=[out_spec, out_spec],
        out_shape=[out, out],
        scratch_shapes=[
            pltpu.VMEM((nmom, 8, LANES), jnp.float32),
            pltpu.VMEM((nmom, 8, LANES), jnp.float32),
            pltpu.VMEM((2, spincol, QX * nvec, LANES), jnp.bfloat16),
            pltpu.VMEM((2, 2, depth, LANES), jnp.bfloat16),
            pltpu.VMEM((2, QX * nvec, 2 * LANES), jnp.float32),
            pltpu.VMEM((nmom, 2, nvec, LANES), jnp.float32),
        ],
        compiler_params=grant(16),
        name="fields",
    )(offset, core, momenta, jnp.asarray(trig_table()), noise, vectors)


def mesons_kernel(scale, part_ref, copies_ref, out_ref, row_ref):
    total = part_ref[0]
    for n in range(1, part_ref.shape[0]):
        total = total + part_ref[n]
    total = total * scale
    for n in range(copies_ref.shape[0]):
        copies_ref[n] = total
    row_ref[...] = total
    for q in range(out_ref.shape[2]):
        for b in range(2):
            r = b * GROUP + q
            for c in range(2):
                out_ref[0, c, q, b : b + 1, :] = row_ref[r : r + 1, c * 64 : (c + 1) * 64]


def summed_mesons(parts, scale, copies, nmom):
    return pl.pallas_call(
        functools.partial(mesons_kernel, scale),
        out_shape=[
            jax.ShapeDtypeStruct((copies, CHUNK, LANES), jnp.float32),
            jax.ShapeDtypeStruct((1, 2, nmom, 2, 64), jnp.float32),
        ],
        scratch_shapes=[pltpu.VMEM((CHUNK, LANES), jnp.float32)],
        compiler_params=grant(4),
        name="mesons",
    )(parts)


def traces_kernel(pairs_ref, fields_ref, out_ref):
    lane = lane_iota(CHUNK)
    sign = jnp.where(lane < 64, -1.0, 1.0)
    re = jnp.zeros((CHUNK, LANES), jnp.float32)
    im = re
    for k in range(pairs_ref.shape[1]):
        source = fields_ref[pairs_ref[0, k]]
        sink = fields_ref[pairs_ref[1, k]]
        swapped = pltpu.roll(source, 64, 1) * sign
        re = jnp.where(lane == k, jnp.sum(sink * source, axis=1, keepdims=True), re)
        im = jnp.where(lane == k, jnp.sum(sink * swapped, axis=1, keepdims=True), im)
    pad = jnp.zeros((64 - CHUNK, LANES), jnp.float32)
    both = jnp.concatenate([re, pad, im, pad], axis=0)
    out_ref[...] = both.T[0:8, :]


def partial_traces(pairs, fields):
    smem = pl.BlockSpec(memory_space=pltpu.SMEM)
    return pl.pallas_call(
        traces_kernel,
        in_specs=[smem, pl.BlockSpec(memory_space=pltpu.VMEM)],
        out_shape=jax.ShapeDtypeStruct((8, LANES), jnp.float32),
        compiler_params=grant(4),
        name="traces",
    )(pairs, fields)


def correlators_kernel(factor, part_ref, out_ref):
    total = part_ref[0]
    for n in range(1, part_ref.shape[0]):
        total = total + part_ref[n]
    total = total * factor
    nmom = out_ref.shape[2]
    total = total + pltpu.roll(total, LANES - GROUP, 1)
    moved = pltpu.roll(total, 64, 1)
    for k in range(out_ref.shape[0]):
        out_ref[k, 0:1, :] = total[k : k + 1, 0:nmom]
        out_ref[k, 1:2, :] = moved[k : k + 1, 0:nmom]


def summed_traces(parts, factor, npairs, nmom):
    return pl.pallas_call(
        functools.partial(correlators_kernel, factor),
        out_shape=jax.ShapeDtypeStruct((npairs, 2, nmom), jnp.float32),
        compiler_params=grant(4),
        name="correlators",
    )(parts)


def exchange(array, axis):
    return lax.all_to_all(array, axis, split_axis=0, concat_axis=0, tiled=True)


def local(solutions, noise, momenta, pairs):
    spincol, sites, width = solutions.shape[1:]
    nmom = momenta.shape[0]
    core = lax.axis_index("core")
    place = lax.axis_index(("z", "yh", "core"))
    offset = (place * sites).astype(jnp.int32).reshape(1)
    peer, own = partial_fields(offset, core.astype(jnp.int32).reshape(1), momenta.T, jnp.swapaxes(noise[0], 0, 1), solutions[0])
    arrived = lax.ppermute(peer, "core", [(0, 1), (1, 0)])
    chunks = (own + arrived).reshape(ZY, CHUNK, LANES)
    scale = 1.0 / math.sqrt(spincol * sites * 2 * ZY)
    copies, mesons = summed_mesons(exchange(chunks, ("z", "yh")), scale, lax.axis_size("tm"), nmom)
    traces = partial_traces(pairs.T, exchange(copies, "tm"))
    traces = traces + lax.ppermute(traces, "core", [(0, 1), (1, 0)])
    spread = jnp.broadcast_to(traces, (ZY, *traces.shape))
    correlators = summed_traces(exchange(spread, ("z", "yh")), 1.0 / 64, pairs.shape[0], nmom)
    return (mesons, correlators)


def solution(mesh):
    split = Mesh(mesh.devices.reshape(8, 2, 2, 8), ("z", "yh", "core", "tm"))
    space = ("z", "yh", "core")
    in_specs = (P("tm", None, space, None), P("tm", None, None, space), P(), P("tm", None))
    out_specs = (P("tm", None, None, space, None), P("tm", None, None))
    return jax.shard_map(local, mesh=split, in_specs=in_specs, out_specs=out_specs, check_vma=False)
```

```python
import functools
import math

import jax
import jax.numpy as jnp
import numpy as np
from jax import lax
from jax.experimental import pallas as pl
from jax.experimental.pallas import tpu as pltpu
from jax.sharding import Mesh
from jax.sharding import PartitionSpec as P

EXTENT = 48
LANES = 128
SITE_BLOCK = 64
QX = 5
ZY = 16
GROUP = 28
CHUNK = 2 * GROUP


def grant(mebibytes):
    return pltpu.CompilerParams(vmem_limit_bytes=mebibytes << 20)


def trig_table():
    angle = (np.arange(LANES) % EXTENT) * (2.0 * np.pi / EXTENT)
    rows = np.stack([np.cos(angle), np.sin(angle)]).astype(np.float32)
    return np.repeat(rows, 8, axis=0)


def lane_iota(rows):
    return lax.broadcasted_iota(jnp.int32, (rows, LANES), 1)


def looked_up(table, index):
    return jnp.take_along_axis(table, index, axis=1)


def field_kernel(mom_hbm, table_hbm, noise_hbm, vec_hbm, peer_ref, own_ref, mom_ref, table_ref, noise_ref, vec_ref, phase_re, phase_im, d_ref, sems):
    nmom = mom_ref.shape[1]
    steps, spincol, nvec = noise_ref.shape[:3]
    core = lax.axis_index("core")
    place = (lax.axis_index("z") * 2 + lax.axis_index("yh")) * 2 + core
    offset = place * (steps * LANES)

    small = [
        pltpu.make_async_copy(mom_hbm, mom_ref, sems.at[0, 0]),
        pltpu.make_async_copy(table_hbm, table_ref, sems.at[1, 0]),
    ]
    blocks = []
    for step in range(steps):
        span = pl.ds(step * LANES, LANES)
        blocks.append(
            [
                pltpu.make_async_copy(noise_hbm.at[:, :, span], noise_ref.at[step], sems.at[0, step + 1]),
                pltpu.make_async_copy(vec_hbm.at[:, span, :], vec_ref.at[step], sems.at[1, step + 1]),
            ]
        )
    for copy in small + sum(blocks, []):
        copy.start()
    for copy in small:
        copy.wait()

    cos_table = table_ref[0:8, :]
    sin_table = table_ref[8:16, :]
    lane8 = lane_iota(8)
    low8 = lane8 < SITE_BLOCK
    low64 = lane_iota(64) < SITE_BLOCK

    first = offset + SITE_BLOCK * lax.broadcasted_iota(jnp.int32, (8, LANES), 0)
    line = lax.div(first, EXTENT) + jnp.where(low8, 0, 1)
    y, z = (lax.rem(line, EXTENT), lax.div(line, EXTENT))
    for q in range(nmom):
        index = mom_ref[1, q] * y + mom_ref[2, q] * z
        index = jnp.where(index < 0, index + 3 * EXTENT, index)
        index = jnp.where(index >= 2 * EXTENT, index - 2 * EXTENT, index)
        phase_re[q] = looked_up(cos_table, index)
        phase_im[q] = -looked_up(sin_table, index)
    zero = jnp.zeros((ZY, LANES), jnp.float32)
    for out in (peer_ref, own_ref):
        for b in range(2):
            out[pl.ds(b * GROUP + GROUP - 1, ZY, stride=CHUNK), :] = zero

    one = jnp.bfloat16(1)
    two = jnp.bfloat16(2)
    site = lax.broadcasted_iota(jnp.int32, (SITE_BLOCK, LANES), 0)
    for step in range(steps):
        waves, masks = ([], [])
        for g in range(2):
            into = lax.rem(offset + (step * 2 + g) * SITE_BLOCK, EXTENT)
            x = into + (lane8 & (SITE_BLOCK - 1))
            x = jnp.where(x >= EXTENT, x - EXTENT, x)
            x2 = 2 * x
            x2 = jnp.where(x2 >= EXTENT, x2 - EXTENT, x2)
            waves.append([looked_up(t, i)[0:1, :].astype(jnp.bfloat16) for i in (x, x2) for t in (cos_table, sin_table)])
            masks.append(jnp.where((site < EXTENT - into) == low64, 1.0, 0.0).astype(jnp.bfloat16))
        for copy in blocks[step]:
            copy.wait()

        totals = [None, None]
        for pair in range(spincol // 2):
            rows = []
            for a in (2 * pair, 2 * pair + 1):
                parts = [noise_ref[step, a, pl.ds(c * 2 + b, ZY, stride=4), :] for c in (1 - core, core) for b in range(2)]
                rows.append(jnp.concatenate(parts, axis=0))
            turned = [pltpu.roll(r, SITE_BLOCK, 1) for r in rows]
            halves = (jnp.where(low64, rows[0], turned[1]), jnp.where(low64, turned[0], rows[1]))
            for g in range(2):
                turns = halves[g].astype(jnp.float32).astype(jnp.bfloat16)
                er = jnp.abs(turns - two) - one
                ei = one - jnp.abs(turns - one)
                left_re = {2: er}
                left_im = {2: -ei}
                for k in (1, 2):
                    c, s = waves[g][2 * (k - 1) : 2 * k]
                    erc, eis, ers, eic = (er * c, ei * s, er * s, ei * c)
                    left_re[2 + k], left_im[2 + k] = (erc - eis, -(ers + eic))
                    left_re[2 - k], left_im[2 - k] = (erc + eis, ers - eic)
                left = [jnp.concatenate([part[n] for n in range(QX)], axis=0) for part in (left_re, left_im)]
                re, im = ([], [])
                for a in (2 * pair, 2 * pair + 1):
                    v = vec_ref[step, a, g * SITE_BLOCK : (g + 1) * SITE_BLOCK, :]
                    swapped = pltpu.roll(v, SITE_BLOCK, 1)
                    re.append(jnp.where(low64, v, swapped) * masks[g])
                    im.append(jnp.where(low64, swapped, v) * masks[g])
                right = [jnp.concatenate(re + [-i for i in im], axis=0), jnp.concatenate(im + re, axis=0)]
                product = jnp.dot(
                    jnp.concatenate(left, axis=1), jnp.concatenate(right, axis=1), preferred_element_type=jnp.float32
                )
                totals[g] = product if totals[g] is None else totals[g] + product
        for g in range(2):
            d_ref[step * 2 + g] = totals[g]

    low = lane_iota(nvec) < SITE_BLOCK
    for q in range(nmom):
        row = pl.multiple_of((mom_ref[0, q] + 2) * nvec, nvec)
        re = im = jnp.zeros((nvec, LANES), jnp.float32)
        for g in range(2 * steps):
            fr = phase_re[q, g : g + 1, :]
            fi = phase_im[q, g : g + 1, :]
            dr = d_ref[g, pl.ds(row, nvec), 0:LANES]
            di = d_ref[g, pl.ds(row, nvec), LANES:]
            re = re + (fr * dr - fi * di)
            im = im + (fr * di + fi * dr)
        total = jnp.where(low, re, im) + pltpu.roll(jnp.where(low, im, re), SITE_BLOCK, 1)
        for n, out in enumerate((peer_ref, own_ref)):
            for b in range(2):
                r = n * 2 * ZY + b * ZY
                out[pl.ds(b * GROUP + q, ZY, stride=CHUNK), :] = total[r : r + ZY]


def partial_fields(momenta, noise, vectors):
    nmom = momenta.shape[1]
    spincol, nvec, sites = noise.shape
    steps = sites // LANES
    out = pltpu.VMEM((ZY * CHUNK, LANES), jnp.float32)
    return pl.pallas_call(
        field_kernel,
        in_specs=[pl.BlockSpec(memory_space=pltpu.HBM)] * 4,
        out_shape=[out, out],
        scratch_shapes=[
            pltpu.SMEM(momenta.shape, jnp.int32),
            pltpu.VMEM((16, LANES), jnp.float32),
            pltpu.VMEM((steps, spincol, nvec, LANES), jnp.int32),
            pltpu.VMEM((steps, spincol, LANES, LANES), jnp.bfloat16),
            pltpu.VMEM((nmom, 8, LANES), jnp.float32),
            pltpu.VMEM((nmom, 8, LANES), jnp.float32),
            pltpu.VMEM((2 * steps, QX * nvec, 2 * LANES), jnp.float32),
            pltpu.SemaphoreType.DMA((2, steps + 1)),
        ],
        compiler_params=grant(24),
        name="fields",
    )(*[pltpu.with_memory_space_constraint(a, pltpu.HBM) for a in (momenta, jnp.asarray(trig_table()), noise, vectors)])


def mesons_kernel(scale, part_ref, copies_ref, out_ref, row_ref):
    total = part_ref[0]
    for n in range(1, part_ref.shape[0]):
        total = total + part_ref[n]
    total = total * scale
    for n in range(copies_ref.shape[0]):
        copies_ref[n] = total
    row_ref[...] = total
    for q in range(out_ref.shape[2]):
        for b in range(2):
            r = b * GROUP + q
            for c in range(2):
                out_ref[0, c, q, b : b + 1, :] = row_ref[r : r + 1, c * 64 : (c + 1) * 64]


def summed_mesons(parts, scale, copies, nmom):
    return pl.pallas_call(
        functools.partial(mesons_kernel, scale),
        out_shape=[
            jax.ShapeDtypeStruct((copies, CHUNK, LANES), jnp.float32),
            jax.ShapeDtypeStruct((1, 2, nmom, 2, 64), jnp.float32),
        ],
        scratch_shapes=[pltpu.VMEM((CHUNK, LANES), jnp.float32)],
        compiler_params=grant(4),
        name="mesons",
    )(parts)


def traces_kernel(pairs_ref, fields_ref, out_ref):
    lane = lane_iota(CHUNK)
    sign = jnp.where(lane < 64, -1.0, 1.0)
    re = jnp.zeros((CHUNK, LANES), jnp.float32)
    im = re
    for k in range(pairs_ref.shape[1]):
        source = fields_ref[pairs_ref[0, k]]
        sink = fields_ref[pairs_ref[1, k]]
        swapped = pltpu.roll(source, 64, 1) * sign
        re = jnp.where(lane == k, jnp.sum(sink * source, axis=1, keepdims=True), re)
        im = jnp.where(lane == k, jnp.sum(sink * swapped, axis=1, keepdims=True), im)
    pad = jnp.zeros((64 - CHUNK, LANES), jnp.float32)
    both = jnp.concatenate([re, pad, im, pad], axis=0)
    out_ref[...] = both.T[0:8, :]


def partial_traces(pairs, fields):
    smem = pl.BlockSpec(memory_space=pltpu.SMEM)
    return pl.pallas_call(
        traces_kernel,
        in_specs=[smem, pl.BlockSpec(memory_space=pltpu.VMEM)],
        out_shape=jax.ShapeDtypeStruct((8, LANES), jnp.float32),
        compiler_params=grant(4),
        name="traces",
    )(pairs, fields)


def correlators_kernel(factor, part_ref, out_ref):
    total = part_ref[0]
    for n in range(1, part_ref.shape[0]):
        total = total + part_ref[n]
    total = total * factor
    nmom = out_ref.shape[2]
    total = total + pltpu.roll(total, LANES - GROUP, 1)
    moved = pltpu.roll(total, 64, 1)
    for k in range(out_ref.shape[0]):
        out_ref[k, 0:1, :] = total[k : k + 1, 0:nmom]
        out_ref[k, 1:2, :] = moved[k : k + 1, 0:nmom]


def summed_traces(parts, factor, npairs, nmom):
    return pl.pallas_call(
        functools.partial(correlators_kernel, factor),
        out_shape=jax.ShapeDtypeStruct((npairs, 2, nmom), jnp.float32),
        compiler_params=grant(4),
        name="correlators",
    )(parts)


def exchange(array, axis):
    return lax.all_to_all(array, axis, split_axis=0, concat_axis=0, tiled=True)


def local(solutions, noise, momenta, pairs):
    spincol, sites, width = solutions.shape[1:]
    nmom = momenta.shape[0]
    peer, own = partial_fields(momenta.T, jnp.swapaxes(noise[0], 0, 1), solutions[0])
    arrived = lax.ppermute(peer, "core", [(0, 1), (1, 0)])
    chunks = (own + arrived).reshape(ZY, CHUNK, LANES)
    scale = 1.0 / math.sqrt(spincol * sites * 2 * ZY)
    copies, mesons = summed_mesons(exchange(chunks, ("z", "yh")), scale, lax.axis_size("tm"), nmom)
    traces = partial_traces(pairs.T, exchange(copies, "tm"))
    traces = traces + lax.ppermute(traces, "core", [(0, 1), (1, 0)])
    spread = jnp.broadcast_to(traces, (ZY, *traces.shape))
    correlators = summed_traces(exchange(spread, ("z", "yh")), 1.0 / 64, pairs.shape[0], nmom)
    return (mesons, correlators)


def solution(mesh):
    split = Mesh(mesh.devices.reshape(8, 2, 2, 8), ("z", "yh", "core", "tm"))
    space = ("z", "yh", "core")
    in_specs = (P("tm", None, space, None), P("tm", None, None, space), P(), P("tm", None))
    out_specs = (P("tm", None, None, space, None), P("tm", None, None))
    return jax.shard_map(local, mesh=split, in_specs=in_specs, out_specs=out_specs, check_vma=False)
```

```python
import functools
import math

import jax
import jax.numpy as jnp
import numpy as np
from jax import lax
from jax.experimental import pallas as pl
from jax.experimental.pallas import tpu as pltpu
from jax.sharding import Mesh
from jax.sharding import PartitionSpec as P

EXTENT = 48
LANES = 128
SITE_BLOCK = 64
QX = 5
Z = 8
ZY = 2 * Z
HALF = 32
GROUP = 28
CHUNK = 2 * GROUP


def grant(mebibytes):
    return pltpu.CompilerParams(vmem_limit_bytes=mebibytes << 20)


def trig_table():
    angle = (np.arange(LANES) % EXTENT) * (2.0 * np.pi / EXTENT)
    rows = np.stack([np.cos(angle), np.sin(angle)]).astype(np.float32)
    return np.repeat(rows, 8, axis=0)


def lane_iota(rows):
    return lax.broadcasted_iota(jnp.int32, (rows, LANES), 1)


def looked_up(table, index):
    return jnp.take_along_axis(table, index, axis=1)


def combined(mom_ref, phase_re, phase_im, d_ref, out_ref):
    low = lane_iota(HALF) < SITE_BLOCK
    for q in range(mom_ref.shape[1]):
        kind = mom_ref[0, q] + 2
        re = im = jnp.zeros((HALF, LANES), jnp.float32)
        for g in range(d_ref.shape[0]):
            fr = phase_re[q, g : g + 1, :]
            fi = phase_im[q, g : g + 1, :]
            dr = d_ref[g, kind, :, 0:LANES]
            di = d_ref[g, kind, :, LANES:]
            re = re + (fr * dr - fi * di)
            im = im + (fr * di + fi * dr)
        total = jnp.where(low, re, im) + pltpu.roll(jnp.where(low, im, re), SITE_BLOCK, 1)
        for y in range(2):
            for b in range(2):
                r = (y * 2 + b) * Z
                out_ref[y, pl.ds(b * GROUP + q, Z, stride=CHUNK), :] = total[r : r + Z]
    for y in range(2):
        for b in range(2):
            out_ref[y, pl.ds(b * GROUP + GROUP - 1, Z, stride=CHUNK), :] = jnp.zeros((Z, LANES), jnp.float32)


def own_kernel(mom_hbm, phase_re, phase_im, d_ref, out_ref, mom_ref, sem):
    copy = pltpu.make_async_copy(mom_hbm, mom_ref, sem)
    copy.start()
    copy.wait()
    combined(mom_ref, phase_re, phase_im, d_ref, out_ref)


def field_kernel(mom_hbm, table_hbm, noise_hbm, vec_hbm, peer_ref, phase_re, phase_im, own_d, mom_ref, table_ref, noise_ref, vec_ref, peer_d, sems):
    nmom = mom_ref.shape[1]
    steps, spincol, nvec = noise_ref.shape[:3]
    core = lax.axis_index("core")
    yh = lax.axis_index("yh")
    place = (lax.axis_index("z") * 2 + yh) * 2 + core
    offset = place * (steps * LANES)

    small = [
        pltpu.make_async_copy(mom_hbm, mom_ref, sems.at[0, 0]),
        pltpu.make_async_copy(table_hbm, table_ref, sems.at[1, 0]),
    ]
    blocks = []
    for step in range(steps):
        span = pl.ds(step * LANES, LANES)
        blocks.append(
            [
                pltpu.make_async_copy(noise_hbm.at[:, :, span], noise_ref.at[step], sems.at[0, step + 1]),
                pltpu.make_async_copy(vec_hbm.at[:, span, :], vec_ref.at[step], sems.at[1, step + 1]),
            ]
        )
    for copy in small + sum(blocks, []):
        copy.start()
    for copy in small:
        copy.wait()

    cos_table = table_ref[0:8, :]
    sin_table = table_ref[8:16, :]
    lane8 = lane_iota(8)
    low8 = lane8 < SITE_BLOCK
    low64 = lane_iota(64) < SITE_BLOCK

    first = offset + SITE_BLOCK * lax.broadcasted_iota(jnp.int32, (8, LANES), 0)
    line = lax.div(first, EXTENT) + jnp.where(low8, 0, 1)
    y, z = (lax.rem(line, EXTENT), lax.div(line, EXTENT))
    for q in range(nmom):
        index = mom_ref[1, q] * y + mom_ref[2, q] * z
        index = jnp.where(index < 0, index + 3 * EXTENT, index)
        index = jnp.where(index >= 2 * EXTENT, index - 2 * EXTENT, index)
        phase_re[q] = looked_up(cos_table, index)
        phase_im[q] = -looked_up(sin_table, index)

    one = jnp.bfloat16(1)
    two = jnp.bfloat16(2)
    site = lax.broadcasted_iota(jnp.int32, (SITE_BLOCK, LANES), 0)
    for step in range(steps):
        waves, masks = ([], [])
        for g in range(2):
            into = lax.rem(offset + (step * 2 + g) * SITE_BLOCK, EXTENT)
            x = into + (lane8 & (SITE_BLOCK - 1))
            x = jnp.where(x >= EXTENT, x - EXTENT, x)
            x2 = 2 * x
            x2 = jnp.where(x2 >= EXTENT, x2 - EXTENT, x2)
            waves.append([looked_up(t, i)[0:1, :].astype(jnp.bfloat16) for i in (x, x2) for t in (cos_table, sin_table)])
            masks.append(jnp.where((site < EXTENT - into) == low64, 1.0, 0.0).astype(jnp.bfloat16))
        for copy in blocks[step]:
            copy.wait()

        totals = [None, None]
        for pair in range(spincol // 2):
            rows = []
            for a in (2 * pair, 2 * pair + 1):
                firsts = [y * 4 + c * 2 + b for c in (1 - core, core) for y in (1 - yh, yh) for b in range(2)]
                parts = [noise_ref[step, a, pl.ds(first, Z, stride=8), :] for first in firsts]
                rows.append(jnp.concatenate(parts, axis=0))
            turned = [pltpu.roll(r, SITE_BLOCK, 1) for r in rows]
            halves = (jnp.where(low64, rows[0], turned[1]), jnp.where(low64, turned[0], rows[1]))
            for g in range(2):
                turns = halves[g].astype(jnp.float32).astype(jnp.bfloat16)
                er = jnp.abs(turns - two) - one
                ei = one - jnp.abs(turns - one)
                left_re = {2: er}
                left_im = {2: -ei}
                for k in (1, 2):
                    c, s = waves[g][2 * (k - 1) : 2 * k]
                    erc, eis, ers, eic = (er * c, ei * s, er * s, ei * c)
                    left_re[2 + k], left_im[2 + k] = (erc - eis, -(ers + eic))
                    left_re[2 - k], left_im[2 - k] = (erc + eis, ers - eic)
                left = [jnp.concatenate([part[n] for n in range(QX)], axis=0) for part in (left_re, left_im)]
                re, im = ([], [])
                for a in (2 * pair, 2 * pair + 1):
                    v = vec_ref[step, a, g * SITE_BLOCK : (g + 1) * SITE_BLOCK, :]
                    swapped = pltpu.roll(v, SITE_BLOCK, 1)
                    re.append(jnp.where(low64, v, swapped) * masks[g])
                    im.append(jnp.where(low64, swapped, v) * masks[g])
                right = [jnp.concatenate(re + [-i for i in im], axis=0), jnp.concatenate(im + re, axis=0)]
                product = jnp.dot(
                    jnp.concatenate(left, axis=1), jnp.concatenate(right, axis=1), preferred_element_type=jnp.float32
                )
                totals[g] = product if totals[g] is None else totals[g] + product
        for g in range(2):
            for n in range(QX):
                peer_d[step * 2 + g, n] = totals[g][n * nvec : n * nvec + HALF]
                own_d[step * 2 + g, n] = totals[g][n * nvec + HALF : (n + 1) * nvec]

    combined(mom_ref, phase_re, phase_im, peer_d, peer_ref)


def in_hbm(array):
    return pltpu.with_memory_space_constraint(array, pltpu.HBM)


def partial_fields(momenta, noise, vectors):
    nmom = momenta.shape[1]
    spincol, nvec, sites = noise.shape
    steps = sites // LANES
    rows = pltpu.VMEM((2, Z * CHUNK, LANES), jnp.float32)
    phase = pltpu.VMEM((nmom, 8, LANES), jnp.float32)
    lines = pltpu.VMEM((2 * steps, QX, HALF, 2 * LANES), jnp.float32)
    hbm = pl.BlockSpec(memory_space=pltpu.HBM)
    vmem = pl.BlockSpec(memory_space=pltpu.VMEM)
    momenta = in_hbm(momenta)
    peer, *rest = pl.pallas_call(
        field_kernel,
        in_specs=[hbm] * 4,
        out_specs=[vmem] * 4,
        out_shape=[rows, phase, phase, lines],
        scratch_shapes=[
            pltpu.SMEM(momenta.shape, jnp.int32),
            pltpu.VMEM((16, LANES), jnp.float32),
            pltpu.VMEM((steps, spincol, nvec, LANES), jnp.int32),
            pltpu.VMEM((steps, spincol, LANES, LANES), jnp.bfloat16),
            lines,
            pltpu.SemaphoreType.DMA((2, steps + 1)),
        ],
        compiler_params=grant(24),
        name="fields",
    )(momenta, in_hbm(jnp.asarray(trig_table())), in_hbm(noise), in_hbm(vectors))
    own = pl.pallas_call(
        own_kernel,
        in_specs=[hbm] + [vmem] * 3,
        out_specs=vmem,
        out_shape=rows,
        scratch_shapes=[pltpu.SMEM(momenta.shape, jnp.int32), pltpu.SemaphoreType.DMA],
        compiler_params=grant(8),
        name="own",
    )(momenta, *[pltpu.with_memory_space_constraint(a, pltpu.VMEM) for a in rest])
    return (peer, own)


def mesons_kernel(scale, part_ref, copies_ref, out_ref, row_ref):
    total = part_ref[0]
    for n in range(1, part_ref.shape[0]):
        total = total + part_ref[n]
    total = total * scale
    for n in range(copies_ref.shape[0]):
        copies_ref[n] = total
    row_ref[...] = total
    for q in range(out_ref.shape[2]):
        for b in range(2):
            r = b * GROUP + q
            for c in range(2):
                out_ref[0, c, q, b : b + 1, :] = row_ref[r : r + 1, c * 64 : (c + 1) * 64]


def summed_mesons(parts, scale, copies, nmom):
    return pl.pallas_call(
        functools.partial(mesons_kernel, scale),
        out_shape=[
            jax.ShapeDtypeStruct((copies, CHUNK, LANES), jnp.float32),
            pltpu.VMEM((1, 2, nmom, 2, 64), jnp.float32),
        ],
        scratch_shapes=[pltpu.VMEM((CHUNK, LANES), jnp.float32)],
        compiler_params=grant(4),
        name="mesons",
    )(parts)


def traces_kernel(pairs_ref, mesons_ref, fields_ref, out_ref, mesons_hbm, sem):
    copy = pltpu.make_async_copy(mesons_ref, mesons_hbm, sem)
    copy.start()
    lane = lane_iota(CHUNK)
    sign = jnp.where(lane < 64, -1.0, 1.0)
    re = jnp.zeros((CHUNK, LANES), jnp.float32)
    im = re
    for k in range(pairs_ref.shape[1]):
        source = fields_ref[pairs_ref[0, k]]
        sink = fields_ref[pairs_ref[1, k]]
        swapped = pltpu.roll(source, 64, 1) * sign
        re = jnp.where(lane == k, jnp.sum(sink * source, axis=1, keepdims=True), re)
        im = jnp.where(lane == k, jnp.sum(sink * swapped, axis=1, keepdims=True), im)
    pad = jnp.zeros((64 - CHUNK, LANES), jnp.float32)
    both = jnp.concatenate([re, pad, im, pad], axis=0)
    out_ref[...] = both.T[0:8, :]
    copy.wait()


def partial_traces(pairs, mesons, fields):
    vmem = pl.BlockSpec(memory_space=pltpu.VMEM)
    return pl.pallas_call(
        traces_kernel,
        in_specs=[pl.BlockSpec(memory_space=pltpu.SMEM), vmem, vmem],
        out_specs=[vmem, pl.BlockSpec(memory_space=pltpu.HBM)],
        out_shape=[pltpu.VMEM((8, LANES), jnp.float32), pltpu.HBM(mesons.shape, jnp.float32)],
        scratch_shapes=[pltpu.SemaphoreType.DMA],
        compiler_params=grant(4),
        name="traces",
    )(pairs, mesons, fields)


def correlators_kernel(factor, part_ref, out_ref):
    total = part_ref[0]
    for n in range(1, part_ref.shape[0]):
        total = total + part_ref[n]
    total = total * factor
    nmom = out_ref.shape[2]
    total = total + pltpu.roll(total, LANES - GROUP, 1)
    moved = pltpu.roll(total, 64, 1)
    for k in range(out_ref.shape[0]):
        out_ref[k, 0:1, :] = total[k : k + 1, 0:nmom]
        out_ref[k, 1:2, :] = moved[k : k + 1, 0:nmom]


def summed_traces(parts, factor, npairs, nmom):
    return pl.pallas_call(
        functools.partial(correlators_kernel, factor),
        out_shape=jax.ShapeDtypeStruct((npairs, 2, nmom), jnp.float32),
        compiler_params=grant(4),
        name="correlators",
    )(parts)


def exchange(array, axis):
    return lax.all_to_all(array, axis, split_axis=0, concat_axis=0, tiled=True)


def local(solutions, noise, momenta, pairs):
    spincol, sites, width = solutions.shape[1:]
    nmom = momenta.shape[0]
    peer, own = partial_fields(momenta.T, jnp.swapaxes(noise[0], 0, 1), solutions[0])
    arrived = lax.ppermute(peer, "core", [(0, 1), (1, 0)])
    theirs = lax.ppermute(own[0] + arrived[0], "yh", [(0, 1), (1, 0)])
    chunks = (own[1] + arrived[1] + theirs).reshape(Z, CHUNK, LANES)
    scale = 1.0 / math.sqrt(spincol * sites * 2 * ZY)
    copies, mesons = summed_mesons(exchange(chunks, "z"), scale, lax.axis_size("tm"), nmom)
    traces, mesons = partial_traces(pairs.T, mesons, exchange(copies, "tm"))
    traces = traces + lax.ppermute(traces, "core", [(0, 1), (1, 0)])
    spread = jnp.broadcast_to(traces, (ZY, *traces.shape))
    correlators = summed_traces(exchange(spread, ("z", "yh")), 1.0 / 64, pairs.shape[0], nmom)
    return (mesons, correlators)


def solution(mesh):
    split = Mesh(mesh.devices.reshape(8, 2, 2, 8), ("z", "yh", "core", "tm"))
    space = ("z", "yh", "core")
    in_specs = (P("tm", None, space, None), P("tm", None, None, space), P(), P("tm", None))
    out_specs = (P("tm", None, None, space, None), P("tm", None, None))
    return jax.shard_map(local, mesh=split, in_specs=in_specs, out_specs=out_specs, check_vma=False)
```

```python
import functools
import math

import jax
import jax.numpy as jnp
import numpy as np
from jax import lax
from jax.experimental import pallas as pl
from jax.experimental.pallas import tpu as pltpu
from jax.sharding import Mesh
from jax.sharding import PartitionSpec as P

EXTENT = 48
LANES = 128
SITE_BLOCK = 64
QX = 5
ZY = 16
HALF = 32
GROUP = 28
BLOCK = 2 * GROUP


def grant(mebibytes):
    return pltpu.CompilerParams(vmem_limit_bytes=mebibytes << 20)


def trig_table():
    angle = (np.arange(LANES) % EXTENT) * (2.0 * np.pi / EXTENT)
    rows = np.stack([np.cos(angle), np.sin(angle)]).astype(np.float32)
    return np.repeat(rows, 8, axis=0)


def lane_iota(rows):
    return lax.broadcasted_iota(jnp.int32, (rows, LANES), 1)


def looked_up(table, index):
    return jnp.take_along_axis(table, index, axis=1)


def combined(mom_ref, phase_re, phase_im, d_ref, out_ref):
    nmom = mom_ref.shape[1]
    low = lane_iota(HALF) < SITE_BLOCK
    for q in range(nmom):
        kind = mom_ref[0, q] + 2
        re = im = jnp.zeros((HALF, LANES), jnp.float32)
        for g in range(d_ref.shape[0]):
            fr = phase_re[q, g : g + 1, :]
            fi = phase_im[q, g : g + 1, :]
            dr = d_ref[g, kind, :, 0:LANES]
            di = d_ref[g, kind, :, LANES:]
            re = re + (fr * dr - fi * di)
            im = im + (fr * di + fi * dr)
        total = jnp.where(low, re, im) + pltpu.roll(jnp.where(low, im, re), SITE_BLOCK, 1)
        for b in range(2):
            out_ref[pl.ds(b * GROUP + q, ZY, stride=BLOCK), :] = total[b * ZY : (b + 1) * ZY]
    for row in range(nmom, BLOCK, GROUP):
        out_ref[pl.ds(row, ZY, stride=BLOCK), :] = jnp.zeros((ZY, LANES), jnp.float32)


def own_kernel(mom_hbm, phase_re, phase_im, d_ref, out_ref, mom_ref, sem):
    copy = pltpu.make_async_copy(mom_hbm, mom_ref, sem)
    copy.start()
    copy.wait()
    combined(mom_ref, phase_re, phase_im, d_ref, out_ref)


def field_kernel(mom_hbm, table_hbm, noise_hbm, vec_hbm, peer_ref, phase_re, phase_im, own_d, mom_ref, table_ref, noise_ref, vec_ref, peer_d, sems):
    nmom = mom_ref.shape[1]
    steps, spincol, nvec = noise_ref.shape[:3]
    core = lax.axis_index("core")
    place = (lax.axis_index("z") * 2 + lax.axis_index("yh")) * 2 + core
    offset = place * (steps * LANES)

    small = [
        pltpu.make_async_copy(mom_hbm, mom_ref, sems.at[0, 0]),
        pltpu.make_async_copy(table_hbm, table_ref, sems.at[1, 0]),
    ]
    blocks = []
    for step in range(steps):
        span = pl.ds(step * LANES, LANES)
        blocks.append(
            [
                pltpu.make_async_copy(noise_hbm.at[:, :, span], noise_ref.at[step], sems.at[0, step + 1]),
                pltpu.make_async_copy(vec_hbm.at[:, span, :], vec_ref.at[step], sems.at[1, step + 1]),
            ]
        )
    for copy in small + sum(blocks, []):
        copy.start()
    for copy in small:
        copy.wait()

    cos_table = table_ref[0:8, :]
    sin_table = table_ref[8:16, :]
    lane8 = lane_iota(8)
    low8 = lane8 < SITE_BLOCK
    low64 = lane_iota(64) < SITE_BLOCK

    first = offset + SITE_BLOCK * lax.broadcasted_iota(jnp.int32, (8, LANES), 0)
    line = lax.div(first, EXTENT) + jnp.where(low8, 0, 1)
    y, z = (lax.rem(line, EXTENT), lax.div(line, EXTENT))
    for q in range(nmom):
        index = mom_ref[1, q] * y + mom_ref[2, q] * z
        index = jnp.where(index < 0, index + 3 * EXTENT, index)
        index = jnp.where(index >= 2 * EXTENT, index - 2 * EXTENT, index)
        phase_re[q] = looked_up(cos_table, index)
        phase_im[q] = -looked_up(sin_table, index)

    one = jnp.bfloat16(1)
    two = jnp.bfloat16(2)
    site = lax.broadcasted_iota(jnp.int32, (SITE_BLOCK, LANES), 0)
    for step in range(steps):
        waves, masks = ([], [])
        for g in range(2):
            into = lax.rem(offset + (step * 2 + g) * SITE_BLOCK, EXTENT)
            x = into + (lane8 & (SITE_BLOCK - 1))
            x = jnp.where(x >= EXTENT, x - EXTENT, x)
            x2 = 2 * x
            x2 = jnp.where(x2 >= EXTENT, x2 - EXTENT, x2)
            waves.append([looked_up(t, i)[0:1, :].astype(jnp.bfloat16) for i in (x, x2) for t in (cos_table, sin_table)])
            masks.append(jnp.where((site < EXTENT - into) == low64, 1.0, 0.0).astype(jnp.bfloat16))
        for copy in blocks[step]:
            copy.wait()

        totals = [None, None]
        for pair in range(spincol // 2):
            rows = []
            for a in (2 * pair, 2 * pair + 1):
                firsts = [c * 2 + b for c in (1 - core, core) for b in range(2)]
                parts = [noise_ref[step, a, pl.ds(first, ZY, stride=4), :] for first in firsts]
                rows.append(jnp.concatenate(parts, axis=0))
            turned = [pltpu.roll(r, SITE_BLOCK, 1) for r in rows]
            halves = (jnp.where(low64, rows[0], turned[1]), jnp.where(low64, turned[0], rows[1]))
            for g in range(2):
                turns = halves[g].astype(jnp.float32).astype(jnp.bfloat16)
                er = jnp.abs(turns - two) - one
                ei = jnp.abs(turns - one) - one
                left_re, left_im = ([er], [ei])
                for k in (1, 2):
                    c, s = waves[g][2 * (k - 1) : 2 * k]
                    minus_s = -s
                    left_re += [er * c, ei * s]
                    left_im += [ei * c, er * minus_s]
                left = [jnp.concatenate(part, axis=0) for part in (left_re, left_im)]
                re, im = ([], [])
                for a in (2 * pair, 2 * pair + 1):
                    v = vec_ref[step, a, g * SITE_BLOCK : (g + 1) * SITE_BLOCK, :]
                    swapped = pltpu.roll(v, SITE_BLOCK, 1)
                    re.append(jnp.where(low64, v, swapped) * masks[g])
                    im.append(jnp.where(low64, swapped, v) * masks[g])
                right = [jnp.concatenate(re + [-i for i in im], axis=0), jnp.concatenate(im + re, axis=0)]
                product = jnp.dot(
                    jnp.concatenate(left, axis=1), jnp.concatenate(right, axis=1), preferred_element_type=jnp.float32
                )
                totals[g] = product if totals[g] is None else totals[g] + product
        for g in range(2):
            for rows, lines in ((slice(0, HALF), peer_d), (slice(HALF, nvec), own_d)):
                parts = [totals[g][n * nvec : (n + 1) * nvec][rows] for n in range(QX)]
                at = step * 2 + g
                lines[at, 2] = parts[0]
                for k in (1, 2):
                    lines[at, 2 + k] = parts[2 * k - 1] + parts[2 * k]
                    lines[at, 2 - k] = parts[2 * k - 1] - parts[2 * k]

    combined(mom_ref, phase_re, phase_im, peer_d, peer_ref)


def in_hbm(array):
    return pltpu.with_memory_space_constraint(array, pltpu.HBM)


def partial_fields(momenta, noise, vectors):
    nmom = momenta.shape[1]
    spincol, nvec, sites = noise.shape
    steps = sites // LANES
    rows = pltpu.VMEM((ZY * BLOCK, LANES), jnp.float32)
    phase = pltpu.VMEM((nmom, 8, LANES), jnp.float32)
    lines = pltpu.VMEM((2 * steps, QX, HALF, 2 * LANES), jnp.float32)
    hbm = pl.BlockSpec(memory_space=pltpu.HBM)
    vmem = pl.BlockSpec(memory_space=pltpu.VMEM)
    momenta = in_hbm(momenta)
    peer, *rest = pl.pallas_call(
        field_kernel,
        in_specs=[hbm] * 4,
        out_specs=[vmem] * 4,
        out_shape=[rows, phase, phase, lines],
        scratch_shapes=[
            pltpu.SMEM(momenta.shape, jnp.int32),
            pltpu.VMEM((16, LANES), jnp.float32),
            pltpu.VMEM((steps, spincol, nvec, LANES), jnp.int32),
            pltpu.VMEM((steps, spincol, LANES, LANES), jnp.bfloat16),
            lines,
            pltpu.SemaphoreType.DMA((2, steps + 1)),
        ],
        compiler_params=grant(24),
        name="fields",
    )(momenta, in_hbm(jnp.asarray(trig_table())), in_hbm(noise), in_hbm(vectors))
    own = pl.pallas_call(
        own_kernel,
        in_specs=[hbm] + [vmem] * 3,
        out_specs=vmem,
        out_shape=rows,
        scratch_shapes=[pltpu.SMEM(momenta.shape, jnp.int32), pltpu.SemaphoreType.DMA],
        compiler_params=grant(8),
        name="own",
    )(momenta, *[pltpu.with_memory_space_constraint(a, pltpu.VMEM) for a in rest])
    return (peer, own)


def mesons_kernel(scale, part_ref, copies_ref, out_ref, row_ref):
    total = part_ref[0]
    for n in range(1, ZY):
        total = total + part_ref[n]
    total = total * scale
    for n in range(copies_ref.shape[0]):
        copies_ref[n] = total
    row_ref[...] = total
    for q in range(out_ref.shape[2]):
        for b in range(2):
            r = b * GROUP + q
            for c in range(2):
                out_ref[0, c, q, b : b + 1, :] = row_ref[r : r + 1, c * 64 : (c + 1) * 64]


def summed_mesons(parts, scale, copies, nmom):
    return pl.pallas_call(
        functools.partial(mesons_kernel, scale),
        out_shape=[
            pltpu.VMEM((copies, BLOCK, LANES), jnp.float32),
            pltpu.VMEM((1, 2, nmom, 2, 64), jnp.float32),
        ],
        scratch_shapes=[pltpu.VMEM((BLOCK, LANES), jnp.float32)],
        compiler_params=grant(4),
        name="mesons",
    )(parts)


def traces_kernel(pairs_ref, mesons_ref, fields_ref, out_ref, mesons_hbm, sem):
    copy = pltpu.make_async_copy(mesons_ref, mesons_hbm, sem)
    copy.start()
    lane = lane_iota(BLOCK)
    sign = jnp.where(lane < 64, -1.0, 1.0)
    re = jnp.zeros((BLOCK, LANES), jnp.float32)
    im = re
    for k in range(pairs_ref.shape[1]):
        source = fields_ref[pairs_ref[0, k]]
        sink = fields_ref[pairs_ref[1, k]]
        swapped = pltpu.roll(source, 64, 1) * sign
        re = jnp.where(lane == k, jnp.sum(sink * source, axis=1, keepdims=True), re)
        im = jnp.where(lane == k, jnp.sum(sink * swapped, axis=1, keepdims=True), im)
    re = re[0:32] + pltpu.roll(re, BLOCK - GROUP, 0)[0:32]
    im = im[0:32] + pltpu.roll(im, BLOCK - GROUP, 0)[0:32]
    pad = jnp.zeros((64, LANES), jnp.float32)
    both = jnp.concatenate([re, im, pad], axis=0).T
    out_ref[...] = both[0:4] + pltpu.roll(both, 64, 1)[4:8]
    copy.wait()


def partial_traces(pairs, mesons, fields):
    vmem = pl.BlockSpec(memory_space=pltpu.VMEM)
    return pl.pallas_call(
        traces_kernel,
        in_specs=[pl.BlockSpec(memory_space=pltpu.SMEM), vmem, vmem],
        out_specs=[vmem, pl.BlockSpec(memory_space=pltpu.HBM)],
        out_shape=[pltpu.VMEM((4, LANES), jnp.float32), pltpu.HBM(mesons.shape, jnp.float32)],
        scratch_shapes=[pltpu.SemaphoreType.DMA],
        compiler_params=grant(4),
        name="traces",
    )(pairs, mesons, fields)


def correlators_kernel(factor, part_ref, out_ref):
    total = part_ref[0]
    for n in range(1, part_ref.shape[0]):
        total = total + part_ref[n]
    total = total * factor
    nmom = out_ref.shape[2]
    for k in range(out_ref.shape[0]):
        for c in range(2):
            first = (k // 4) * 64 + c * 32
            moved = total if first == 0 else pltpu.roll(total, LANES - first, 1)
            out_ref[k, c : c + 1, :] = moved[k % 4 : k % 4 + 1, 0:nmom]


def summed_traces(parts, factor, npairs, nmom):
    return pl.pallas_call(
        functools.partial(correlators_kernel, factor),
        out_shape=jax.ShapeDtypeStruct((npairs, 2, nmom), jnp.float32),
        compiler_params=grant(4),
        name="correlators",
    )(parts)


def exchange(array, axis):
    return lax.all_to_all(array, axis, split_axis=0, concat_axis=0, tiled=True)


def local(solutions, noise, momenta, pairs):
    spincol, sites, width = solutions.shape[1:]
    nmom = momenta.shape[0]
    peer, own = partial_fields(momenta.T, jnp.swapaxes(noise[0], 0, 1), solutions[0])
    arrived = lax.ppermute(peer, "core", [(0, 1), (1, 0)])
    scale = 1.0 / math.sqrt(spincol * sites * 2 * ZY)
    copies, mesons = summed_mesons(exchange((own + arrived).reshape(ZY, BLOCK, LANES), ("z", "yh")), scale, lax.axis_size("tm"), nmom)
    traces, mesons = partial_traces(pairs.T, mesons, exchange(copies, "tm"))
    traces = traces + lax.ppermute(traces, "core", [(0, 1), (1, 0)])
    spread = jnp.broadcast_to(traces, (ZY, *traces.shape))
    correlators = summed_traces(exchange(spread, ("z", "yh")), 1.0 / 64, pairs.shape[0], nmom)
    return (mesons, correlators)


def solution(mesh):
    split = Mesh(mesh.devices.reshape(8, 2, 2, 8), ("z", "yh", "core", "tm"))
    space = ("z", "yh", "core")
    in_specs = (P("tm", None, space, None), P("tm", None, None, space), P(), P("tm", None))
    out_specs = (P("tm", None, None, space, None), P("tm", None, None))
    return jax.shard_map(local, mesh=split, in_specs=in_specs, out_specs=out_specs, check_vma=False)
```

```python
import functools
import math

import jax
import jax.numpy as jnp
import numpy as np
from jax import lax
from jax.experimental import pallas as pl
from jax.experimental.pallas import tpu as pltpu
from jax.sharding import Mesh
from jax.sharding import PartitionSpec as P

EXTENT = 48
LANES = 128
SITE_BLOCK = 64
QX = 5
ZY = 16
HALF = 32
GROUP = 28
BLOCK = 2 * GROUP
FACTORS = (1.624205, 1.13242)


def grant(mebibytes):
    return pltpu.CompilerParams(vmem_limit_bytes=mebibytes << 20)


def trig_table():
    angle = (np.arange(LANES) % EXTENT) * (2.0 * np.pi / EXTENT)
    rows = np.stack([np.cos(angle), np.sin(angle)]).astype(np.float32)
    return np.repeat(rows, 8, axis=0)


def lane_iota(rows):
    return lax.broadcasted_iota(jnp.int32, (rows, LANES), 1)


def looked_up(table, index):
    return jnp.take_along_axis(table, index, axis=1)


def combined(mom_ref, phase_re, phase_im, lines, first_block, out_ref, sums_ref=None, last=True, part=None):
    nmom = mom_ref.shape[1]
    low = lane_iota(HALF) < SITE_BLOCK
    for q in range(*(part or (0, nmom))):
        kind = mom_ref[0, q] + 2
        if first_block == 0:
            re = im = jnp.zeros((HALF, LANES), jnp.float32)
        else:
            re, im = (sums_ref[q, 0], sums_ref[q, 1])
        for g in range(lines.shape[0]):
            fr = phase_re[q, first_block + g : first_block + g + 1, :]
            fi = phase_im[q, first_block + g : first_block + g + 1, :]
            dr = lines[g, kind, :, 0:LANES]
            di = lines[g, kind, :, LANES:]
            re = re + (fr * dr - fi * di)
            im = im + (fr * di + fi * dr)
        if not last:
            sums_ref[q, 0] = re
            sums_ref[q, 1] = im
            continue
        total = jnp.where(low, re, im) + pltpu.roll(jnp.where(low, im, re), SITE_BLOCK, 1)
        for b in range(2):
            out_ref[pl.ds(b * GROUP + q, ZY, stride=BLOCK), :] = total[b * ZY : (b + 1) * ZY]
    if last:
        for row in range(nmom, BLOCK, GROUP):
            out_ref[pl.ds(row, ZY, stride=BLOCK), :] = jnp.zeros((ZY, LANES), jnp.float32)


def own_kernel(mom_hbm, phase_re, phase_im, d_ref, out_ref, mom_ref, sem):
    copy = pltpu.make_async_copy(mom_hbm, mom_ref, sem)
    copy.start()
    copy.wait()
    combined(mom_ref, phase_re, phase_im, d_ref, 0, out_ref)


def field_kernel(mom_hbm, table_hbm, noise_hbm, vec_hbm, peer_ref, phase_re, phase_im, own_d, mom_ref, table_ref, noise_ref, vec_ref, even_d, odd_d, sums_ref, sems):
    nmom = mom_ref.shape[1]
    steps, spincol, nvec = noise_ref.shape[:3]
    core = lax.axis_index("core")
    place = (lax.axis_index("z") * 2 + lax.axis_index("yh")) * 2 + core
    offset = place * (steps * LANES)

    small = [
        pltpu.make_async_copy(mom_hbm, mom_ref, sems.at[0, 0]),
        pltpu.make_async_copy(table_hbm, table_ref, sems.at[1, 0]),
    ]
    blocks = []
    for step in range(steps):
        span = pl.ds(step * LANES, LANES)
        blocks.append(
            [
                pltpu.make_async_copy(noise_hbm.at[:, :, span], noise_ref.at[step], sems.at[0, step + 1]),
                pltpu.make_async_copy(vec_hbm.at[:, span, :], vec_ref.at[step], sems.at[1, step + 1]),
            ]
        )
    for copy in small + sum(blocks, []):
        copy.start()
    for copy in small:
        copy.wait()

    cos_table = table_ref[0:8, :]
    sin_table = table_ref[8:16, :]
    lane8 = lane_iota(8)
    low8 = lane8 < SITE_BLOCK
    low64 = lane_iota(64) < SITE_BLOCK

    first = offset + SITE_BLOCK * lax.broadcasted_iota(jnp.int32, (8, LANES), 0)
    line = lax.div(first, EXTENT) + jnp.where(low8, 0, 1)
    y, z = (lax.rem(line, EXTENT), lax.div(line, EXTENT))
    for q in range(nmom):
        index = mom_ref[1, q] * y + mom_ref[2, q] * z
        index = jnp.where(index < 0, index + 3 * EXTENT, index)
        index = jnp.where(index >= 2 * EXTENT, index - 2 * EXTENT, index)
        kind = jnp.abs(mom_ref[0, q])
        undo = jnp.where(kind == 0, 1.0, jnp.where(kind == 1, 1.0 / FACTORS[0], 1.0 / FACTORS[1]))
        phase_re[q] = looked_up(cos_table, index) * undo
        phase_im[q] = -looked_up(sin_table, index) * undo

    one = jnp.bfloat16(1)
    two = jnp.bfloat16(2)
    site = lax.broadcasted_iota(jnp.int32, (SITE_BLOCK, LANES), 0)
    for step in range(steps):
        waves, masks = ([], [])
        for g in range(2):
            into = lax.rem(offset + (step * 2 + g) * SITE_BLOCK, EXTENT)
            x = into + (lane8 & (SITE_BLOCK - 1))
            x = jnp.where(x >= EXTENT, x - EXTENT, x)
            x2 = 2 * x
            x2 = jnp.where(x2 >= EXTENT, x2 - EXTENT, x2)
            waves.append(
                [
                    (looked_up(t, i)[0:1, :] * f).astype(jnp.bfloat16)
                    for i, f in zip((x, x2), FACTORS, strict=True)
                    for t in (cos_table, sin_table)
                ]
            )
            masks.append(jnp.where((site < EXTENT - into) == low64, 1.0, 0.0).astype(jnp.bfloat16))
        for copy in [] if step > 1 else blocks[0] if step == 0 else sum(blocks[1:], []):
            copy.wait()
        lines, before = (odd_d, even_d) if step % 2 else (even_d, odd_d)

        totals = [None, None]
        each = -(-nmom // (spincol // 2))
        for pair in range(spincol // 2):
            if step > 0:
                part = (pair * each, min(nmom, (pair + 1) * each))
                combined(mom_ref, phase_re, phase_im, before, 2 * step - 2, peer_ref, sums_ref, last=False, part=part)
            rows = []
            for a in (2 * pair, 2 * pair + 1):
                firsts = [c * 2 + b for c in (1 - core, core) for b in range(2)]
                parts = [noise_ref[step, a, pl.ds(first, ZY, stride=4), :] for first in firsts]
                rows.append(jnp.concatenate(parts, axis=0))
            turned = [pltpu.roll(r, SITE_BLOCK, 1) for r in rows]
            halves = (jnp.where(low64, rows[0], turned[1]), jnp.where(low64, turned[0], rows[1]))
            for g in range(2):
                turns = halves[g].astype(jnp.float32).astype(jnp.bfloat16)
                er = jnp.abs(turns - two) - one
                ei = jnp.abs(turns - one) - one
                left_re, left_im = ([er], [ei])
                for k in (1, 2):
                    c, s = waves[g][2 * (k - 1) : 2 * k]
                    minus_s = -s
                    left_re += [er * c, ei * s]
                    left_im += [ei * c, er * minus_s]
                left = [jnp.concatenate(part, axis=0) for part in (left_re, left_im)]
                re, im = ([], [])
                for a in (2 * pair, 2 * pair + 1):
                    v = vec_ref[step, a, g * SITE_BLOCK : (g + 1) * SITE_BLOCK, :]
                    swapped = pltpu.roll(v, SITE_BLOCK, 1)
                    re.append(jnp.where(low64, v, swapped) * masks[g])
                    im.append(jnp.where(low64, swapped, v) * masks[g])
                right = [jnp.concatenate(re + [-i for i in im], axis=0), jnp.concatenate(im + re, axis=0)]
                product = jnp.dot(
                    jnp.concatenate(left, axis=1), jnp.concatenate(right, axis=1), preferred_element_type=jnp.float32
                )
                totals[g] = product if totals[g] is None else totals[g] + product
        for g in range(2):
            parts = [totals[g][n * nvec : (n + 1) * nvec] for n in range(QX)]
            values = {2: parts[0]}
            for k in (1, 2):
                values[2 + k] = parts[2 * k - 1] + parts[2 * k]
                values[2 - k] = parts[2 * k - 1] - parts[2 * k]
            for n in range(QX):
                lines[g, n] = values[n][:HALF]
                own_d[step * 2 + g, n] = values[n][HALF:]

    combined(mom_ref, phase_re, phase_im, lines, 2 * steps - 2, peer_ref, sums_ref)


def in_hbm(array):
    return pltpu.with_memory_space_constraint(array, pltpu.HBM)


def partial_fields(momenta, noise, vectors):
    nmom = momenta.shape[1]
    spincol, nvec, sites = noise.shape
    steps = sites // LANES
    rows = pltpu.VMEM((ZY * BLOCK, LANES), jnp.float32)
    phase = pltpu.VMEM((nmom, 8, LANES), jnp.float32)
    lines = pltpu.VMEM((2 * steps, QX, HALF, 2 * LANES), jnp.float32)
    hbm = pl.BlockSpec(memory_space=pltpu.HBM)
    vmem = pl.BlockSpec(memory_space=pltpu.VMEM)
    momenta = in_hbm(momenta)
    peer, *rest = pl.pallas_call(
        field_kernel,
        in_specs=[hbm] * 4,
        out_specs=[vmem] * 4,
        out_shape=[rows, phase, phase, lines],
        scratch_shapes=[
            pltpu.SMEM(momenta.shape, jnp.int32),
            pltpu.VMEM((16, LANES), jnp.float32),
            pltpu.VMEM((steps, spincol, nvec, LANES), jnp.int32),
            pltpu.VMEM((steps, spincol, LANES, LANES), jnp.bfloat16),
            pltpu.VMEM((2, QX, HALF, 2 * LANES), jnp.float32),
            pltpu.VMEM((2, QX, HALF, 2 * LANES), jnp.float32),
            pltpu.VMEM((nmom, 2, HALF, LANES), jnp.float32),
            pltpu.SemaphoreType.DMA((2, steps + 1)),
        ],
        compiler_params=grant(24),
        name="fields",
    )(momenta, in_hbm(jnp.asarray(trig_table())), in_hbm(noise), in_hbm(vectors))
    own = pl.pallas_call(
        own_kernel,
        in_specs=[hbm] + [vmem] * 3,
        out_specs=vmem,
        out_shape=rows,
        scratch_shapes=[pltpu.SMEM(momenta.shape, jnp.int32), pltpu.SemaphoreType.DMA],
        compiler_params=grant(8),
        name="own",
    )(momenta, *[pltpu.with_memory_space_constraint(a, pltpu.VMEM) for a in rest])
    return (peer, own)


def mesons_kernel(scale, part_ref, copies_ref, out_ref, row_ref):
    total = part_ref[0]
    for n in range(1, ZY):
        total = total + part_ref[n]
    total = total * scale
    for n in range(copies_ref.shape[0]):
        copies_ref[n] = total
    row_ref[...] = total
    for q in range(out_ref.shape[2]):
        for b in range(2):
            r = b * GROUP + q
            for c in range(2):
                out_ref[0, c, q, b : b + 1, :] = row_ref[r : r + 1, c * 64 : (c + 1) * 64]


def summed_mesons(parts, scale, copies, nmom):
    return pl.pallas_call(
        functools.partial(mesons_kernel, scale),
        out_shape=[
            pltpu.VMEM((copies, BLOCK, LANES), jnp.float32),
            pltpu.VMEM((1, 2, nmom, 2, 64), jnp.float32),
        ],
        scratch_shapes=[pltpu.VMEM((BLOCK, LANES), jnp.float32)],
        compiler_params=grant(4),
        name="mesons",
    )(parts)


def traces_kernel(pairs_ref, mesons_ref, fields_ref, out_ref, mesons_hbm, sem):
    copy = pltpu.make_async_copy(mesons_ref, mesons_hbm, sem)
    copy.start()
    lane = lane_iota(BLOCK)
    sign = jnp.where(lane < 64, -1.0, 1.0)
    re = jnp.zeros((BLOCK, LANES), jnp.float32)
    im = re
    for k in range(pairs_ref.shape[1]):
        source = fields_ref[pairs_ref[0, k]]
        sink = fields_ref[pairs_ref[1, k]]
        swapped = pltpu.roll(source, 64, 1) * sign
        re = jnp.where(lane == k, jnp.sum(sink * source, axis=1, keepdims=True), re)
        im = jnp.where(lane == k, jnp.sum(sink * swapped, axis=1, keepdims=True), im)
    re = re[0:32] + pltpu.roll(re, BLOCK - GROUP, 0)[0:32]
    im = im[0:32] + pltpu.roll(im, BLOCK - GROUP, 0)[0:32]
    pad = jnp.zeros((64, LANES), jnp.float32)
    both = jnp.concatenate([re, im, pad], axis=0).T
    out_ref[...] = both[0:4] + pltpu.roll(both, 64, 1)[4:8]
    copy.wait()


def partial_traces(pairs, mesons, fields):
    vmem = pl.BlockSpec(memory_space=pltpu.VMEM)
    return pl.pallas_call(
        traces_kernel,
        in_specs=[pl.BlockSpec(memory_space=pltpu.SMEM), vmem, vmem],
        out_specs=[vmem, pl.BlockSpec(memory_space=pltpu.HBM)],
        out_shape=[pltpu.VMEM((4, LANES), jnp.float32), pltpu.HBM(mesons.shape, jnp.float32)],
        scratch_shapes=[pltpu.SemaphoreType.DMA],
        compiler_params=grant(4),
        name="traces",
    )(pairs, mesons, fields)


def correlators_kernel(factor, part_ref, out_ref):
    total = part_ref[0]
    for n in range(1, part_ref.shape[0]):
        total = total + part_ref[n]
    total = total * factor
    nmom = out_ref.shape[2]
    for k in range(out_ref.shape[0]):
        for c in range(2):
            first = (k // 4) * 64 + c * 32
            moved = total if first == 0 else pltpu.roll(total, LANES - first, 1)
            out_ref[k, c : c + 1, :] = moved[k % 4 : k % 4 + 1, 0:nmom]


def summed_traces(parts, factor, npairs, nmom):
    return pl.pallas_call(
        functools.partial(correlators_kernel, factor),
        out_shape=jax.ShapeDtypeStruct((npairs, 2, nmom), jnp.float32),
        compiler_params=grant(4),
        name="correlators",
    )(parts)


def exchange(array, axis):
    return lax.all_to_all(array, axis, split_axis=0, concat_axis=0, tiled=True)


def local(solutions, noise, momenta, pairs):
    spincol, sites, width = solutions.shape[1:]
    nmom = momenta.shape[0]
    peer, own = partial_fields(momenta.T, jnp.swapaxes(noise[0], 0, 1), solutions[0])
    arrived = lax.ppermute(peer, "core", [(0, 1), (1, 0)])
    scale = 1.0 / math.sqrt(spincol * sites * 2 * ZY)
    copies, mesons = summed_mesons(exchange((own + arrived).reshape(ZY, BLOCK, LANES), ("z", "yh")), scale, lax.axis_size("tm"), nmom)
    traces, mesons = partial_traces(pairs.T, mesons, exchange(copies, "tm"))
    traces = traces + lax.ppermute(traces, "core", [(0, 1), (1, 0)])
    spread = jnp.broadcast_to(traces, (ZY, *traces.shape))
    correlators = summed_traces(exchange(spread, ("z", "yh")), 1.0 / 64, pairs.shape[0], nmom)
    return (mesons, correlators)


def solution(mesh):
    split = Mesh(mesh.devices.reshape(8, 2, 2, 8), ("z", "yh", "core", "tm"))
    space = ("z", "yh", "core")
    in_specs = (P("tm", None, space, None), P("tm", None, None, space), P(), P("tm", None))
    out_specs = (P("tm", None, None, space, None), P("tm", None, None))
    return jax.shard_map(local, mesh=split, in_specs=in_specs, out_specs=out_specs, check_vma=False)
```

```python
import functools
import math

import jax
import jax.numpy as jnp
import numpy as np
from jax import lax
from jax.experimental import pallas as pl
from jax.experimental.pallas import tpu as pltpu
from jax.sharding import Mesh
from jax.sharding import PartitionSpec as P

EXTENT = 48
LANES = 128
SITE_BLOCK = 64
QX = 5
ZY = 16
HALF = 32
GROUP = 28
BLOCK = 2 * GROUP
FACTORS = (1.624205, 1.13242)


def grant(mebibytes):
    return pltpu.CompilerParams(vmem_limit_bytes=mebibytes << 20)


def trig_table():
    angle = (np.arange(LANES) % EXTENT) * (2.0 * np.pi / EXTENT)
    rows = np.stack([np.cos(angle), np.sin(angle)]).astype(np.float32)
    return np.repeat(rows, 8, axis=0)


def lane_iota(rows):
    return lax.broadcasted_iota(jnp.int32, (rows, LANES), 1)


def looked_up(table, index):
    return jnp.take_along_axis(table, index, axis=1)


def combined(mom_ref, phase_re, phase_im, lines, first_block, out_ref, sums_ref=None, last=True, part=None):
    nmom = mom_ref.shape[1]
    low = lane_iota(HALF) < SITE_BLOCK
    for q in range(*(part or (0, nmom))):
        kind = mom_ref[0, q] + 2
        if first_block == 0:
            re = im = jnp.zeros((HALF, LANES), jnp.float32)
        else:
            re, im = (sums_ref[q, 0], sums_ref[q, 1])
        for g in range(lines.shape[0]):
            fr = phase_re[q, first_block + g : first_block + g + 1, :]
            fi = phase_im[q, first_block + g : first_block + g + 1, :]
            dr = lines[g, kind, :, 0:LANES]
            di = lines[g, kind, :, LANES:]
            re = re + (fr * dr - fi * di)
            im = im + (fr * di + fi * dr)
        if not last:
            sums_ref[q, 0] = re
            sums_ref[q, 1] = im
            continue
        total = jnp.where(low, re, im) + pltpu.roll(jnp.where(low, im, re), SITE_BLOCK, 1)
        for b in range(2):
            out_ref[pl.ds(b * GROUP + q, ZY, stride=BLOCK), :] = total[b * ZY : (b + 1) * ZY]
    if last:
        for row in range(nmom, BLOCK, GROUP):
            out_ref[pl.ds(row, ZY, stride=BLOCK), :] = jnp.zeros((ZY, LANES), jnp.float32)


def own_kernel(mom_ref, phase_re, phase_im, d_ref, out_ref):
    combined(mom_ref[...], phase_re, phase_im, d_ref, 0, out_ref)


def field_kernel(mom_hbm, table_hbm, noise_hbm, vec_hbm, peer_ref, phase_re, phase_im, own_d, mom_ref, table_ref, noise_ref, vec_ref, even_d, odd_d, sums_ref, sems):
    nmom = mom_ref.shape[1]
    steps, spincol, nvec = noise_ref.shape[:3]
    core = lax.axis_index("core")
    place = (lax.axis_index("z") * 2 + lax.axis_index("yh")) * 2 + core
    offset = place * (steps * LANES)

    small = [
        pltpu.make_async_copy(mom_hbm, mom_ref, sems.at[0, 0]),
        pltpu.make_async_copy(table_hbm, table_ref, sems.at[1, 0]),
    ]
    blocks = []
    for step in range(steps):
        span = pl.ds(step * LANES, LANES)
        blocks.append(
            [
                pltpu.make_async_copy(noise_hbm.at[:, :, span], noise_ref.at[step], sems.at[0, step + 1]),
                pltpu.make_async_copy(vec_hbm.at[:, span, :], vec_ref.at[step], sems.at[1, step + 1]),
            ]
        )
    for copy in small + sum(blocks, []):
        copy.start()
    for copy in small:
        copy.wait()

    cos_table = table_ref[0:8, :]
    sin_table = table_ref[8:16, :]
    lane8 = lane_iota(8)
    low8 = lane8 < SITE_BLOCK
    low64 = lane_iota(64) < SITE_BLOCK

    first = offset + SITE_BLOCK * lax.broadcasted_iota(jnp.int32, (8, LANES), 0)
    line = lax.div(first, EXTENT) + jnp.where(low8, 0, 1)
    y, z = (lax.rem(line, EXTENT), lax.div(line, EXTENT))
    for q in range(nmom):
        index = mom_ref[1, q] * y + mom_ref[2, q] * z
        index = jnp.where(index < 0, index + 3 * EXTENT, index)
        index = jnp.where(index >= 2 * EXTENT, index - 2 * EXTENT, index)
        kind = jnp.abs(mom_ref[0, q])
        undo = jnp.where(kind == 0, 1.0, jnp.where(kind == 1, 1.0 / FACTORS[0], 1.0 / FACTORS[1]))
        phase_re[q] = looked_up(cos_table, index) * undo
        phase_im[q] = -looked_up(sin_table, index) * undo

    one = jnp.bfloat16(1)
    two = jnp.bfloat16(2)
    site = lax.broadcasted_iota(jnp.int32, (SITE_BLOCK, LANES), 0)
    for step in range(steps):
        waves, masks = ([], [])
        for g in range(2):
            into = lax.rem(offset + (step * 2 + g) * SITE_BLOCK, EXTENT)
            x = into + (lane8 & (SITE_BLOCK - 1))
            x = jnp.where(x >= EXTENT, x - EXTENT, x)
            x2 = 2 * x
            x2 = jnp.where(x2 >= EXTENT, x2 - EXTENT, x2)
            waves.append(
                [
                    (looked_up(t, i)[0:1, :] * f).astype(jnp.bfloat16)
                    for i, f in zip((x, x2), FACTORS, strict=True)
                    for t in (cos_table, sin_table)
                ]
            )
            masks.append(jnp.where((site < EXTENT - into) == low64, 1.0, 0.0).astype(jnp.bfloat16))
        for copy in [] if step > 1 else blocks[0] if step == 0 else sum(blocks[1:], []):
            copy.wait()
        lines, before = (odd_d, even_d) if step % 2 else (even_d, odd_d)

        totals = [None, None]
        each = -(-nmom // (spincol // 2))
        for pair in range(spincol // 2):
            if step > 0:
                part = (pair * each, min(nmom, (pair + 1) * each))
                combined(mom_ref, phase_re, phase_im, before, 2 * step - 2, peer_ref, sums_ref, last=False, part=part)
            rows = []
            for a in (2 * pair, 2 * pair + 1):
                firsts = [c * 2 + b for c in (1 - core, core) for b in range(2)]
                parts = [noise_ref[step, a, pl.ds(first, ZY, stride=4), :] for first in firsts]
                rows.append(jnp.concatenate(parts, axis=0))
            turned = [pltpu.roll(r, SITE_BLOCK, 1) for r in rows]
            halves = (jnp.where(low64, rows[0], turned[1]), jnp.where(low64, turned[0], rows[1]))
            for g in range(2):
                turns = halves[g].astype(jnp.float32).astype(jnp.bfloat16)
                er = jnp.abs(turns - two) - one
                ei = jnp.abs(turns - one) - one
                left_re, left_im = ([er], [ei])
                for k in (1, 2):
                    c, s = waves[g][2 * (k - 1) : 2 * k]
                    minus_s = -s
                    left_re += [er * c, ei * s]
                    left_im += [ei * c, er * minus_s]
                left = [jnp.concatenate(part, axis=0) for part in (left_re, left_im)]
                re, im = ([], [])
                for a in (2 * pair, 2 * pair + 1):
                    v = vec_ref[step, a, g * SITE_BLOCK : (g + 1) * SITE_BLOCK, :]
                    swapped = pltpu.roll(v, SITE_BLOCK, 1)
                    re.append(jnp.where(low64, v, swapped) * masks[g])
                    im.append(jnp.where(low64, swapped, v) * masks[g])
                right = [jnp.concatenate(re + [-i for i in im], axis=0), jnp.concatenate(im + re, axis=0)]
                product = jnp.dot(
                    jnp.concatenate(left, axis=1), jnp.concatenate(right, axis=1), preferred_element_type=jnp.float32
                )
                totals[g] = product if totals[g] is None else totals[g] + product
        for g in range(2):
            parts = [totals[g][n * nvec : (n + 1) * nvec] for n in range(QX)]
            values = {2: parts[0]}
            for k in (1, 2):
                values[2 + k] = parts[2 * k - 1] + parts[2 * k]
                values[2 - k] = parts[2 * k - 1] - parts[2 * k]
            for n in range(QX):
                lines[g, n] = values[n][:HALF]
                own_d[step * 2 + g, n] = values[n][HALF:]

    combined(mom_ref, phase_re, phase_im, lines, 2 * steps - 2, peer_ref, sums_ref)


def in_hbm(array):
    return pltpu.with_memory_space_constraint(array, pltpu.HBM)


def partial_fields(momenta, noise, vectors):
    nmom = momenta.shape[1]
    spincol, nvec, sites = noise.shape
    steps = sites // LANES
    rows = pltpu.VMEM((ZY * BLOCK, LANES), jnp.float32)
    phase = pltpu.VMEM((nmom, 8, LANES), jnp.float32)
    lines = pltpu.VMEM((2 * steps, QX, HALF, 2 * LANES), jnp.float32)
    hbm = pl.BlockSpec(memory_space=pltpu.HBM)
    vmem = pl.BlockSpec(memory_space=pltpu.VMEM)
    peer, *rest = pl.pallas_call(
        field_kernel,
        in_specs=[hbm] * 4,
        out_specs=[vmem] * 4,
        out_shape=[rows, phase, phase, lines],
        scratch_shapes=[
            pltpu.SMEM(momenta.shape, jnp.int32),
            pltpu.VMEM((16, LANES), jnp.float32),
            pltpu.VMEM((steps, spincol, nvec, LANES), jnp.int32),
            pltpu.VMEM((steps, spincol, LANES, LANES), jnp.bfloat16),
            pltpu.VMEM((2, QX, HALF, 2 * LANES), jnp.float32),
            pltpu.VMEM((2, QX, HALF, 2 * LANES), jnp.float32),
            pltpu.VMEM((nmom, 2, HALF, LANES), jnp.float32),
            pltpu.SemaphoreType.DMA((2, steps + 1)),
        ],
        compiler_params=grant(24),
        name="fields",
    )(in_hbm(momenta), in_hbm(jnp.asarray(trig_table())), in_hbm(noise), in_hbm(vectors))
    own = pl.pallas_call(
        own_kernel,
        in_specs=[vmem] * 4,
        out_specs=vmem,
        out_shape=rows,
        compiler_params=grant(8),
        name="own",
    )(*[pltpu.with_memory_space_constraint(a, pltpu.VMEM) for a in (momenta, *rest)])
    return (peer, own)


def mesons_kernel(scale, part_ref, copies_ref, out_ref, row_ref):
    total = part_ref[0]
    for n in range(1, ZY):
        total = total + part_ref[n]
    total = total * scale
    for n in range(copies_ref.shape[0]):
        copies_ref[n] = total
    row_ref[...] = total
    for q in range(out_ref.shape[2]):
        for b in range(2):
            r = b * GROUP + q
            for c in range(2):
                out_ref[0, c, q, b : b + 1, :] = row_ref[r : r + 1, c * 64 : (c + 1) * 64]


def summed_mesons(parts, scale, copies, nmom):
    return pl.pallas_call(
        functools.partial(mesons_kernel, scale),
        out_shape=[
            pltpu.VMEM((copies, BLOCK, LANES), jnp.float32),
            pltpu.VMEM((1, 2, nmom, 2, 64), jnp.float32),
        ],
        scratch_shapes=[pltpu.VMEM((BLOCK, LANES), jnp.float32)],
        compiler_params=grant(4),
        name="mesons",
    )(parts)


def traces_kernel(pairs_ref, mesons_ref, fields_ref, out_ref, mesons_hbm, sem):
    copy = pltpu.make_async_copy(mesons_ref, mesons_hbm, sem)
    copy.start()
    lane = lane_iota(BLOCK)
    sign = jnp.where(lane < 64, -1.0, 1.0)
    re = jnp.zeros((BLOCK, LANES), jnp.float32)
    im = re
    pairs = pairs_ref[...]
    for k in range(pairs_ref.shape[1]):
        source = fields_ref[pairs[0, k]]
        sink = fields_ref[pairs[1, k]]
        swapped = pltpu.roll(source, 64, 1) * sign
        re = jnp.where(lane == k, jnp.sum(sink * source, axis=1, keepdims=True), re)
        im = jnp.where(lane == k, jnp.sum(sink * swapped, axis=1, keepdims=True), im)
    re = re[0:32] + pltpu.roll(re, BLOCK - GROUP, 0)[0:32]
    im = im[0:32] + pltpu.roll(im, BLOCK - GROUP, 0)[0:32]
    pad = jnp.zeros((64, LANES), jnp.float32)
    both = jnp.concatenate([re, im, pad], axis=0).T
    out_ref[...] = both[0:4] + pltpu.roll(both, 64, 1)[4:8]
    copy.wait()


def partial_traces(pairs, mesons, fields):
    vmem = pl.BlockSpec(memory_space=pltpu.VMEM)
    return pl.pallas_call(
        traces_kernel,
        in_specs=[vmem, vmem, vmem],
        out_specs=[vmem, pl.BlockSpec(memory_space=pltpu.HBM)],
        out_shape=[pltpu.VMEM((4, LANES), jnp.float32), pltpu.HBM(mesons.shape, jnp.float32)],
        scratch_shapes=[pltpu.SemaphoreType.DMA],
        compiler_params=grant(4),
        name="traces",
    )(pairs, mesons, fields)


def correlators_kernel(factor, part_ref, out_ref):
    total = part_ref[0]
    for n in range(1, part_ref.shape[0]):
        total = total + part_ref[n]
    total = total * factor
    nmom = out_ref.shape[2]
    for k in range(out_ref.shape[0]):
        for c in range(2):
            first = (k // 4) * 64 + c * 32
            moved = total if first == 0 else pltpu.roll(total, LANES - first, 1)
            out_ref[k, c : c + 1, :] = moved[k % 4 : k % 4 + 1, 0:nmom]


def summed_traces(parts, factor, npairs, nmom):
    return pl.pallas_call(
        functools.partial(correlators_kernel, factor),
        out_shape=jax.ShapeDtypeStruct((npairs, 2, nmom), jnp.float32),
        compiler_params=grant(4),
        name="correlators",
    )(parts)


def exchange(array, axis):
    return lax.all_to_all(array, axis, split_axis=0, concat_axis=0, tiled=True)


def local(solutions, noise, momenta, pairs):
    spincol, sites, width = solutions.shape[1:]
    nmom = momenta.shape[0]
    peer, own = partial_fields(momenta.T, jnp.swapaxes(noise[0], 0, 1), solutions[0])
    arrived = lax.ppermute(peer, "core", [(0, 1), (1, 0)])
    scale = 1.0 / math.sqrt(spincol * sites * 2 * ZY)
    copies, mesons = summed_mesons(exchange((own + arrived).reshape(ZY, BLOCK, LANES), ("z", "yh")), scale, lax.axis_size("tm"), nmom)
    traces, mesons = partial_traces(pairs.T, mesons, exchange(copies, "tm"))
    traces = traces + lax.ppermute(traces, "core", [(0, 1), (1, 0)])
    spread = jnp.broadcast_to(traces, (ZY, *traces.shape))
    correlators = summed_traces(exchange(spread, ("z", "yh")), 1.0 / 64, pairs.shape[0], nmom)
    return (mesons, correlators)


def solution(mesh):
    split = Mesh(mesh.devices.reshape(8, 2, 2, 8), ("z", "yh", "core", "tm"))
    space = ("z", "yh", "core")
    in_specs = (P("tm", None, space, None), P("tm", None, None, space), P(), P("tm", None))
    out_specs = (P("tm", None, None, space, None), P("tm", None, None))
    return jax.shard_map(local, mesh=split, in_specs=in_specs, out_specs=out_specs, check_vma=False)
```

```python
import functools
import math

import jax
import jax.numpy as jnp
import numpy as np
from jax import lax
from jax.experimental import pallas as pl
from jax.experimental.pallas import tpu as pltpu
from jax.sharding import Mesh
from jax.sharding import PartitionSpec as P

EXTENT = 48
LANES = 128
SITE_BLOCK = 64
QX = 5
ZY = 16
HALF = 32
GROUP = 28
BLOCK = 2 * GROUP
FACTORS = (1.624205, 1.13242)


def grant(mebibytes):
    return pltpu.CompilerParams(vmem_limit_bytes=mebibytes << 20)


def trig_table():
    angle = (np.arange(LANES) % EXTENT) * (2.0 * np.pi / EXTENT)
    rows = np.stack([np.cos(angle), np.sin(angle)]).astype(np.float32)
    return np.repeat(rows, 8, axis=0)


def lane_iota(rows):
    return lax.broadcasted_iota(jnp.int32, (rows, LANES), 1)


def looked_up(table, index):
    return jnp.take_along_axis(table, index, axis=1)


def combined(mom_ref, phase_re, phase_im, lines, first_block, out_ref, sums_ref=None, last=True, part=None):
    nmom = mom_ref.shape[1]
    low = lane_iota(HALF) < SITE_BLOCK
    for q in range(*(part or (0, nmom))):
        kind = mom_ref[0, q] + 2
        if first_block == 0:
            re = im = jnp.zeros((HALF, LANES), jnp.float32)
        else:
            re, im = (sums_ref[q, 0], sums_ref[q, 1])
        for g in range(lines.shape[0]):
            fr = phase_re[q, first_block + g : first_block + g + 1, :]
            fi = phase_im[q, first_block + g : first_block + g + 1, :]
            dr = lines[g, kind, :, 0:LANES]
            di = lines[g, kind, :, LANES:]
            re = re + (fr * dr - fi * di)
            im = im + (fr * di + fi * dr)
        if not last:
            sums_ref[q, 0] = re
            sums_ref[q, 1] = im
            continue
        total = jnp.where(low, re, im) + pltpu.roll(jnp.where(low, im, re), SITE_BLOCK, 1)
        for b in range(2):
            out_ref[pl.ds(b * GROUP + q, ZY, stride=BLOCK), :] = total[b * ZY : (b + 1) * ZY]
    if last:
        for row in range(nmom, BLOCK, GROUP):
            out_ref[pl.ds(row, ZY, stride=BLOCK), :] = jnp.zeros((ZY, LANES), jnp.float32)


def own_kernel(mom_ref, phase_re, phase_im, d_ref, out_ref):
    combined(mom_ref[...], phase_re, phase_im, d_ref, 0, out_ref)


def field_kernel(mom_hbm, table_hbm, noise_hbm, vec_hbm, peer_ref, phase_re, phase_im, own_d, mom_ref, table_ref, noise_ref, vec_ref, even_d, odd_d, sums_ref, sems):
    nmom = mom_ref.shape[1]
    steps, spincol, nvec = noise_ref.shape[:3]
    core = lax.axis_index("core")
    place = (lax.axis_index("z") * 2 + lax.axis_index("yh")) * 2 + core
    offset = place * (steps * LANES)

    small = [
        pltpu.make_async_copy(mom_hbm, mom_ref, sems.at[0, 0]),
        pltpu.make_async_copy(table_hbm, table_ref, sems.at[1, 0]),
    ]
    blocks = []
    for step in range(steps):
        span = pl.ds(step * LANES, LANES)
        blocks.append(
            [
                pltpu.make_async_copy(noise_hbm.at[:, :, span], noise_ref.at[step], sems.at[0, step + 1]),
                pltpu.make_async_copy(vec_hbm.at[:, span, :], vec_ref.at[step], sems.at[1, step + 1]),
            ]
        )
    for copy in small + sum(blocks, []):
        copy.start()
    for copy in small:
        copy.wait()

    cos_table = table_ref[0:8, :]
    sin_table = table_ref[8:16, :]
    lane8 = lane_iota(8)
    low8 = lane8 < SITE_BLOCK
    low64 = lane_iota(64) < SITE_BLOCK

    first = offset + SITE_BLOCK * lax.broadcasted_iota(jnp.int32, (8, LANES), 0)
    line = lax.div(first, EXTENT) + jnp.where(low8, 0, 1)
    y, z = (lax.rem(line, EXTENT), lax.div(line, EXTENT))
    for q in range(nmom):
        index = mom_ref[1, q] * y + mom_ref[2, q] * z
        index = jnp.where(index < 0, index + 3 * EXTENT, index)
        index = jnp.where(index >= 2 * EXTENT, index - 2 * EXTENT, index)
        kind = jnp.abs(mom_ref[0, q])
        undo = jnp.where(kind == 0, 1.0, jnp.where(kind == 1, 1.0 / FACTORS[0], 1.0 / FACTORS[1]))
        phase_re[q] = looked_up(cos_table, index) * undo
        phase_im[q] = -looked_up(sin_table, index) * undo

    one = jnp.bfloat16(1)
    two = jnp.bfloat16(2)
    site = lax.broadcasted_iota(jnp.int32, (SITE_BLOCK, LANES), 0)
    for step in range(steps):
        waves, masks = ([], [])
        for g in range(2):
            into = lax.rem(offset + (step * 2 + g) * SITE_BLOCK, EXTENT)
            x = into + (lane8 & (SITE_BLOCK - 1))
            x = jnp.where(x >= EXTENT, x - EXTENT, x)
            x2 = 2 * x
            x2 = jnp.where(x2 >= EXTENT, x2 - EXTENT, x2)
            waves.append(
                [
                    (looked_up(t, i)[0:1, :] * f).astype(jnp.bfloat16)
                    for i, f in zip((x, x2), FACTORS, strict=True)
                    for t in (cos_table, sin_table)
                ]
            )
            masks.append(jnp.where((site < EXTENT - into) == low64, 1.0, 0.0).astype(jnp.bfloat16))
        for copy in [] if step > 1 else blocks[0] if step == 0 else sum(blocks[1:], []):
            copy.wait()
        lines, before = (odd_d, even_d) if step % 2 else (even_d, odd_d)

        totals = [None, None]
        each = -(-nmom // (spincol // 2))
        for pair in range(spincol // 2):
            if step > 0:
                part = (pair * each, min(nmom, (pair + 1) * each))
                combined(mom_ref, phase_re, phase_im, before, 2 * step - 2, peer_ref, sums_ref, last=False, part=part)
            rows = []
            for a in (2 * pair, 2 * pair + 1):
                firsts = [c * 2 + b for c in (1 - core, core) for b in range(2)]
                parts = [noise_ref[step, a, pl.ds(first, ZY, stride=4), :] for first in firsts]
                rows.append(jnp.concatenate(parts, axis=0).astype(jnp.float32).astype(jnp.bfloat16))
            turned = [pltpu.roll(r, SITE_BLOCK, 1) for r in rows]
            halves = (jnp.where(low64, rows[0], turned[1]), jnp.where(low64, turned[0], rows[1]))
            for g in range(2):
                turns = halves[g]
                er = jnp.abs(turns - two) - one
                ei = jnp.abs(turns - one) - one
                left_re, left_im = ([er], [ei])
                for k in (1, 2):
                    c, s = waves[g][2 * (k - 1) : 2 * k]
                    minus_s = -s
                    left_re += [er * c, ei * s]
                    left_im += [ei * c, er * minus_s]
                left = [jnp.concatenate(part, axis=0) for part in (left_re, left_im)]
                re, im = ([], [])
                for a in (2 * pair, 2 * pair + 1):
                    v = vec_ref[step, a, g * SITE_BLOCK : (g + 1) * SITE_BLOCK, :]
                    swapped = pltpu.roll(v, SITE_BLOCK, 1)
                    re.append(jnp.where(low64, v, swapped) * masks[g])
                    im.append(jnp.where(low64, swapped, v) * masks[g])
                right = [jnp.concatenate(re + [-i for i in im], axis=0), jnp.concatenate(im + re, axis=0)]
                product = jnp.dot(
                    jnp.concatenate(left, axis=1), jnp.concatenate(right, axis=1), preferred_element_type=jnp.float32
                )
                totals[g] = product if totals[g] is None else totals[g] + product
        for g in range(2):
            parts = [totals[g][n * nvec : (n + 1) * nvec] for n in range(QX)]
            values = {2: parts[0]}
            for k in (1, 2):
                values[2 + k] = parts[2 * k - 1] + parts[2 * k]
                values[2 - k] = parts[2 * k - 1] - parts[2 * k]
            for n in range(QX):
                lines[g, n] = values[n][:HALF]
                own_d[step * 2 + g, n] = values[n][HALF:]

    combined(mom_ref, phase_re, phase_im, lines, 2 * steps - 2, peer_ref, sums_ref)


def in_hbm(array):
    return pltpu.with_memory_space_constraint(array, pltpu.HBM)


def partial_fields(momenta, noise, vectors):
    nmom = momenta.shape[1]
    spincol, nvec, sites = noise.shape
    steps = sites // LANES
    rows = pltpu.VMEM((ZY * BLOCK, LANES), jnp.float32)
    phase = pltpu.VMEM((nmom, 8, LANES), jnp.float32)
    lines = pltpu.VMEM((2 * steps, QX, HALF, 2 * LANES), jnp.float32)
    hbm = pl.BlockSpec(memory_space=pltpu.HBM)
    vmem = pl.BlockSpec(memory_space=pltpu.VMEM)
    peer, *rest = pl.pallas_call(
        field_kernel,
        in_specs=[hbm] * 4,
        out_specs=[vmem] * 4,
        out_shape=[rows, phase, phase, lines],
        scratch_shapes=[
            pltpu.SMEM(momenta.shape, jnp.int32),
            pltpu.VMEM((16, LANES), jnp.float32),
            pltpu.VMEM((steps, spincol, nvec, LANES), jnp.int32),
            pltpu.VMEM((steps, spincol, LANES, LANES), jnp.bfloat16),
            pltpu.VMEM((2, QX, HALF, 2 * LANES), jnp.float32),
            pltpu.VMEM((2, QX, HALF, 2 * LANES), jnp.float32),
            pltpu.VMEM((nmom, 2, HALF, LANES), jnp.float32),
            pltpu.SemaphoreType.DMA((2, steps + 1)),
        ],
        compiler_params=grant(24),
        name="fields",
    )(in_hbm(momenta), in_hbm(jnp.asarray(trig_table())), in_hbm(noise), in_hbm(vectors))
    own = pl.pallas_call(
        own_kernel,
        in_specs=[vmem] * 4,
        out_specs=vmem,
        out_shape=rows,
        compiler_params=grant(8),
        name="own",
    )(*[pltpu.with_memory_space_constraint(a, pltpu.VMEM) for a in (momenta, *rest)])
    return (peer, own)


def mesons_kernel(scale, part_ref, copies_ref, out_ref, row_ref):
    total = part_ref[0]
    for n in range(1, ZY):
        total = total + part_ref[n]
    total = total * scale
    for n in range(copies_ref.shape[0]):
        copies_ref[n] = total
    row_ref[...] = total
    for q in range(out_ref.shape[2]):
        for b in range(2):
            r = b * GROUP + q
            for c in range(2):
                out_ref[0, c, q, b : b + 1, :] = row_ref[r : r + 1, c * 64 : (c + 1) * 64]


def summed_mesons(parts, scale, copies, nmom):
    return pl.pallas_call(
        functools.partial(mesons_kernel, scale),
        out_shape=[
            pltpu.VMEM((copies, BLOCK, LANES), jnp.float32),
            pltpu.VMEM((1, 2, nmom, 2, 64), jnp.float32),
        ],
        scratch_shapes=[pltpu.VMEM((BLOCK, LANES), jnp.float32)],
        compiler_params=grant(4),
        name="mesons",
    )(parts)


def traces_kernel(pairs_ref, mesons_ref, fields_ref, out_ref, mesons_hbm, sem):
    copy = pltpu.make_async_copy(mesons_ref, mesons_hbm, sem)
    copy.start()
    lane = lane_iota(BLOCK)
    sign = jnp.where(lane < 64, -1.0, 1.0)
    re = jnp.zeros((BLOCK, LANES), jnp.float32)
    im = re
    pairs = pairs_ref[...]
    for k in range(pairs_ref.shape[1]):
        source = fields_ref[pairs[0, k]]
        sink = fields_ref[pairs[1, k]]
        swapped = pltpu.roll(source, 64, 1) * sign
        re = jnp.where(lane == k, jnp.sum(sink * source, axis=1, keepdims=True), re)
        im = jnp.where(lane == k, jnp.sum(sink * swapped, axis=1, keepdims=True), im)
    re = re[0:32] + pltpu.roll(re, BLOCK - GROUP, 0)[0:32]
    im = im[0:32] + pltpu.roll(im, BLOCK - GROUP, 0)[0:32]
    pad = jnp.zeros((64, LANES), jnp.float32)
    both = jnp.concatenate([re, im, pad], axis=0).T
    out_ref[...] = both[0:4] + pltpu.roll(both, 64, 1)[4:8]
    copy.wait()


def partial_traces(pairs, mesons, fields):
    vmem = pl.BlockSpec(memory_space=pltpu.VMEM)
    return pl.pallas_call(
        traces_kernel,
        in_specs=[vmem, vmem, vmem],
        out_specs=[vmem, pl.BlockSpec(memory_space=pltpu.HBM)],
        out_shape=[pltpu.VMEM((4, LANES), jnp.float32), pltpu.HBM(mesons.shape, jnp.float32)],
        scratch_shapes=[pltpu.SemaphoreType.DMA],
        compiler_params=grant(4),
        name="traces",
    )(pairs, mesons, fields)


def correlators_kernel(factor, part_ref, out_ref):
    total = part_ref[0]
    for n in range(1, part_ref.shape[0]):
        total = total + part_ref[n]
    total = total * factor
    nmom = out_ref.shape[2]
    for k in range(out_ref.shape[0]):
        for c in range(2):
            first = (k // 4) * 64 + c * 32
            moved = total if first == 0 else pltpu.roll(total, LANES - first, 1)
            out_ref[k, c : c + 1, :] = moved[k % 4 : k % 4 + 1, 0:nmom]


def summed_traces(parts, factor, npairs, nmom):
    return pl.pallas_call(
        functools.partial(correlators_kernel, factor),
        out_shape=jax.ShapeDtypeStruct((npairs, 2, nmom), jnp.float32),
        compiler_params=grant(4),
        name="correlators",
    )(parts)


def exchange(array, axis):
    return lax.all_to_all(array, axis, split_axis=0, concat_axis=0, tiled=True)


def local(solutions, noise, momenta, pairs):
    spincol, sites, width = solutions.shape[1:]
    nmom = momenta.shape[0]
    peer, own = partial_fields(momenta.T, jnp.swapaxes(noise[0], 0, 1), solutions[0])
    arrived = lax.ppermute(peer, "core", [(0, 1), (1, 0)])
    scale = 1.0 / math.sqrt(spincol * sites * 2 * ZY)
    copies, mesons = summed_mesons(exchange((own + arrived).reshape(ZY, BLOCK, LANES), ("z", "yh")), scale, lax.axis_size("tm"), nmom)
    traces, mesons = partial_traces(pairs.T, mesons, exchange(copies, "tm"))
    traces = traces + lax.ppermute(traces, "core", [(0, 1), (1, 0)])
    spread = jnp.broadcast_to(traces, (ZY, *traces.shape))
    correlators = summed_traces(exchange(spread, ("z", "yh")), 1.0 / 64, pairs.shape[0], nmom)
    return (mesons, correlators)


def solution(mesh):
    split = Mesh(mesh.devices.reshape(8, 2, 2, 8), ("z", "yh", "core", "tm"))
    space = ("z", "yh", "core")
    in_specs = (P("tm", None, space, None), P("tm", None, None, space), P(), P("tm", None))
    out_specs = (P("tm", None, None, space, None), P("tm", None, None))
    return jax.shard_map(local, mesh=split, in_specs=in_specs, out_specs=out_specs, check_vma=False)
```

```python
import functools
import math

import jax
import jax.numpy as jnp
import numpy as np
from jax import lax
from jax.experimental import pallas as pl
from jax.experimental.pallas import tpu as pltpu
from jax.sharding import Mesh
from jax.sharding import PartitionSpec as P

EXTENT = 48
LANES = 128
SITE_BLOCK = 64
QX = 5
ZY = 16
HALF = 32
GROUP = 28
BLOCK = 2 * GROUP
FACTORS = (1.624205, 1.13242)


def grant(mebibytes):
    return pltpu.CompilerParams(vmem_limit_bytes=mebibytes << 20)


def trig_table():
    angle = (np.arange(LANES) % EXTENT) * (2.0 * np.pi / EXTENT)
    rows = np.stack([np.cos(angle), np.sin(angle)]).astype(np.float32)
    return np.repeat(rows, 8, axis=0)


def lane_iota(rows):
    return lax.broadcasted_iota(jnp.int32, (rows, LANES), 1)


def looked_up(table, index):
    return jnp.take_along_axis(table, index, axis=1)


def combined(mom_ref, phase_re, phase_im, lines, first_block, out_ref, sums_ref=None, last=True, part=None):
    nmom = mom_ref.shape[1]
    low = lane_iota(HALF) < SITE_BLOCK
    for q in range(*(part or (0, nmom))):
        kind = mom_ref[0, q] + 2
        if first_block == 0:
            re = im = jnp.zeros((HALF, LANES), jnp.float32)
        else:
            re, im = (sums_ref[q, 0], sums_ref[q, 1])
        for g in range(lines.shape[0]):
            fr = phase_re[q, first_block + g : first_block + g + 1, :]
            fi = phase_im[q, first_block + g : first_block + g + 1, :]
            dr = lines[g, kind, :, 0:LANES]
            di = lines[g, kind, :, LANES:]
            re = re + (fr * dr - fi * di)
            im = im + (fr * di + fi * dr)
        if not last:
            sums_ref[q, 0] = re
            sums_ref[q, 1] = im
            continue
        total = jnp.where(low, re, im) + pltpu.roll(jnp.where(low, im, re), SITE_BLOCK, 1)
        for b in range(2):
            out_ref[pl.ds(b * GROUP + q, ZY, stride=BLOCK), :] = total[b * ZY : (b + 1) * ZY]
    if last:
        for row in range(nmom, BLOCK, GROUP):
            out_ref[pl.ds(row, ZY, stride=BLOCK), :] = jnp.zeros((ZY, LANES), jnp.float32)


def own_kernel(mom_ref, phase_re, phase_im, d_ref, out_ref):
    combined(mom_ref[...], phase_re, phase_im, d_ref, 0, out_ref)


def field_kernel(mom_hbm, table_hbm, noise_hbm, vec_hbm, peer_ref, phase_re, phase_im, own_d, mom_ref, table_ref, noise_ref, vec_ref, even_d, odd_d, sums_ref, sems):
    nmom = mom_ref.shape[1]
    steps, spincol, nvec = noise_ref.shape[:3]
    core = lax.axis_index("core")
    place = (lax.axis_index("z") * 2 + lax.axis_index("yh")) * 2 + core
    offset = place * (steps * LANES)

    small = [
        pltpu.make_async_copy(mom_hbm, mom_ref, sems.at[0, 0]),
        pltpu.make_async_copy(table_hbm, table_ref, sems.at[1, 0]),
    ]
    blocks = []
    for step in range(steps):
        span = pl.ds(step * LANES, LANES)
        blocks.append(
            [
                pltpu.make_async_copy(noise_hbm.at[:, :, span], noise_ref.at[step], sems.at[0, step + 1]),
                pltpu.make_async_copy(vec_hbm.at[:, span, :], vec_ref.at[step], sems.at[1, step + 1]),
            ]
        )
    for copy in small + sum(blocks, []):
        copy.start()
    for copy in small:
        copy.wait()

    cos_table = table_ref[0:8, :]
    sin_table = table_ref[8:16, :]
    lane8 = lane_iota(8)
    low8 = lane8 < SITE_BLOCK
    low64 = lane_iota(64) < SITE_BLOCK

    first = offset + SITE_BLOCK * lax.broadcasted_iota(jnp.int32, (8, LANES), 0)
    line = lax.div(first, EXTENT) + jnp.where(low8, 0, 1)
    y, z = (lax.rem(line, EXTENT), lax.div(line, EXTENT))
    for q in range(nmom):
        index = mom_ref[1, q] * y + mom_ref[2, q] * z
        index = jnp.where(index < 0, index + 3 * EXTENT, index)
        index = jnp.where(index >= 2 * EXTENT, index - 2 * EXTENT, index)
        kind = jnp.abs(mom_ref[0, q])
        undo = jnp.where(kind == 0, 1.0, jnp.where(kind == 1, 1.0 / FACTORS[0], 1.0 / FACTORS[1]))
        phase_re[q] = looked_up(cos_table, index) * undo
        phase_im[q] = -looked_up(sin_table, index) * undo

    one = jnp.bfloat16(1)
    two = jnp.bfloat16(2)
    site = lax.broadcasted_iota(jnp.int32, (SITE_BLOCK, LANES), 0)
    for step in range(steps):
        waves, masks = ([], [])
        for g in range(2):
            into = lax.rem(offset + (step * 2 + g) * SITE_BLOCK, EXTENT)
            x = into + (lane8 & (SITE_BLOCK - 1))
            x = jnp.where(x >= EXTENT, x - EXTENT, x)
            x2 = 2 * x
            x2 = jnp.where(x2 >= EXTENT, x2 - EXTENT, x2)
            waves.append(
                [
                    (looked_up(t, i)[0:1, :] * f).astype(jnp.bfloat16)
                    for i, f in zip((x, x2), FACTORS, strict=True)
                    for t in (cos_table, sin_table)
                ]
            )
            masks.append(jnp.where((site < EXTENT - into) == low64, 1.0, 0.0).astype(jnp.bfloat16))
        for copy in [] if step > 1 else blocks[0] if step == 0 else sum(blocks[1:], []):
            copy.wait()
        lines, before = (odd_d, even_d) if step % 2 else (even_d, odd_d)

        totals = [None, None]
        each = -(-nmom // (spincol // 2))
        for pair in range(spincol // 2):
            if step > 0:
                part = (pair * each, min(nmom, (pair + 1) * each))
                combined(mom_ref, phase_re, phase_im, before, 2 * step - 2, peer_ref, sums_ref, last=False, part=part)
            rows = []
            for a in (2 * pair, 2 * pair + 1):
                firsts = [c * 2 + b for c in (1 - core, core) for b in range(2)]
                parts = [noise_ref[step, a, pl.ds(first, ZY, stride=4), :] for first in firsts]
                rows.append(jnp.concatenate(parts, axis=0).astype(jnp.float32).astype(jnp.bfloat16))
            turned = [pltpu.roll(r, SITE_BLOCK, 1) for r in rows]
            halves = (jnp.where(low64, rows[0], turned[1]), jnp.where(low64, turned[0], rows[1]))
            for g in range(2):
                turns = halves[g]
                er = jnp.abs(turns - two) - one
                ei = jnp.abs(turns - one) - one
                left_re, left_im = ([er], [ei])
                for k in (1, 2):
                    c, s = waves[g][2 * (k - 1) : 2 * k]
                    minus_s = -s
                    left_re += [er * c, ei * s]
                    left_im += [ei * c, er * minus_s]
                left = [jnp.concatenate(part, axis=0) for part in (left_re, left_im)]
                re, im = ([], [])
                for a in (2 * pair, 2 * pair + 1):
                    v = vec_ref[step, a, g * SITE_BLOCK : (g + 1) * SITE_BLOCK, :]
                    swapped = pltpu.roll(v, SITE_BLOCK, 1)
                    re.append(jnp.where(low64, v, swapped) * masks[g])
                    im.append(jnp.where(low64, swapped, v) * masks[g])
                right = [jnp.concatenate(re + [-i for i in im], axis=0), jnp.concatenate(im + re, axis=0)]
                product = jnp.dot(
                    jnp.concatenate(left, axis=1), jnp.concatenate(right, axis=1), preferred_element_type=jnp.float32
                )
                totals[g] = product if totals[g] is None else totals[g] + product
        for g in range(2):
            parts = [totals[g][n * nvec : (n + 1) * nvec] for n in range(QX)]
            values = {2: parts[0]}
            for k in (1, 2):
                values[2 + k] = parts[2 * k - 1] + parts[2 * k]
                values[2 - k] = parts[2 * k - 1] - parts[2 * k]
            for n in range(QX):
                lines[g, n] = values[n][:HALF]
                own_d[step * 2 + g, n] = values[n][HALF:]

    combined(mom_ref, phase_re, phase_im, lines, 2 * steps - 2, peer_ref, sums_ref)


def in_hbm(array):
    return pltpu.with_memory_space_constraint(array, pltpu.HBM)


def partial_fields(momenta, noise, vectors):
    nmom = momenta.shape[1]
    spincol, nvec, sites = noise.shape
    steps = sites // LANES
    rows = pltpu.VMEM((ZY * BLOCK, LANES), jnp.float32)
    phase = pltpu.VMEM((nmom, 8, LANES), jnp.float32)
    lines = pltpu.VMEM((2 * steps, QX, HALF, 2 * LANES), jnp.float32)
    hbm = pl.BlockSpec(memory_space=pltpu.HBM)
    vmem = pl.BlockSpec(memory_space=pltpu.VMEM)
    peer, *rest = pl.pallas_call(
        field_kernel,
        in_specs=[hbm] * 4,
        out_specs=[vmem] * 4,
        out_shape=[rows, phase, phase, lines],
        scratch_shapes=[
            pltpu.SMEM(momenta.shape, jnp.int32),
            pltpu.VMEM((16, LANES), jnp.float32),
            pltpu.VMEM((steps, spincol, nvec, LANES), jnp.int32),
            pltpu.VMEM((steps, spincol, LANES, LANES), jnp.bfloat16),
            pltpu.VMEM((2, QX, HALF, 2 * LANES), jnp.float32),
            pltpu.VMEM((2, QX, HALF, 2 * LANES), jnp.float32),
            pltpu.VMEM((nmom, 2, HALF, LANES), jnp.float32),
            pltpu.SemaphoreType.DMA((2, steps + 1)),
        ],
        compiler_params=grant(24),
        name="fields",
    )(in_hbm(momenta), in_hbm(jnp.asarray(trig_table())), in_hbm(noise), in_hbm(vectors))
    own = pl.pallas_call(
        own_kernel,
        in_specs=[vmem] * 4,
        out_specs=vmem,
        out_shape=rows,
        compiler_params=grant(8),
        name="own",
    )(*[pltpu.with_memory_space_constraint(a, pltpu.VMEM) for a in (momenta, *rest)])
    return (peer, own)


def mesons_kernel(scale, part_ref, copies_ref, out_ref, row_ref):
    total = part_ref[0]
    for n in range(1, ZY):
        total = total + part_ref[n]
    total = total * scale
    for n in range(copies_ref.shape[0]):
        copies_ref[n] = total
    row_ref[...] = total
    for q in range(out_ref.shape[2]):
        for b in range(2):
            r = b * GROUP + q
            for c in range(2):
                out_ref[0, c, q, b : b + 1, :] = row_ref[r : r + 1, c * 64 : (c + 1) * 64]


def summed_mesons(parts, scale, copies, nmom):
    return pl.pallas_call(
        functools.partial(mesons_kernel, scale),
        out_shape=[
            pltpu.VMEM((copies, BLOCK, LANES), jnp.float32),
            pltpu.VMEM((1, 2, nmom, 2, 64), jnp.float32),
        ],
        scratch_shapes=[pltpu.VMEM((BLOCK, LANES), jnp.float32)],
        compiler_params=grant(4),
        name="mesons",
    )(parts)


def traces_kernel(pairs_ref, mesons_ref, fields_ref, out_ref, mesons_hbm, sem):
    copy = pltpu.make_async_copy(mesons_ref, mesons_hbm, sem)
    copy.start()
    lane = lane_iota(BLOCK)
    sign = jnp.where(lane < 64, -1.0, 1.0)
    re = jnp.zeros((BLOCK, LANES), jnp.float32)
    im = re
    pairs = pairs_ref[...]
    for k in range(pairs_ref.shape[1]):
        source = fields_ref[pairs[0, k]]
        sink = fields_ref[pairs[1, k]]
        swapped = pltpu.roll(source, 64, 1) * sign
        re = jnp.where(lane == k, jnp.sum(sink * source, axis=1, keepdims=True), re)
        im = jnp.where(lane == k, jnp.sum(sink * swapped, axis=1, keepdims=True), im)
    re = re[0:32] + pltpu.roll(re, BLOCK - GROUP, 0)[0:32]
    im = im[0:32] + pltpu.roll(im, BLOCK - GROUP, 0)[0:32]
    pad = jnp.zeros((64, LANES), jnp.float32)
    both = jnp.concatenate([re, im, pad], axis=0).T
    out_ref[...] = both[0:4] + pltpu.roll(both, 64, 1)[4:8]
    copy.wait()


def partial_traces(pairs, mesons, fields):
    vmem = pl.BlockSpec(memory_space=pltpu.VMEM)
    return pl.pallas_call(
        traces_kernel,
        in_specs=[vmem, vmem, vmem],
        out_specs=[vmem, pl.BlockSpec(memory_space=pltpu.HBM)],
        out_shape=[pltpu.VMEM((4, LANES), jnp.float32), pltpu.HBM(mesons.shape, jnp.float32)],
        scratch_shapes=[pltpu.SemaphoreType.DMA],
        compiler_params=grant(4),
        name="traces",
    )(pairs, mesons, fields)


def correlators_kernel(factor, part_ref, out_ref):
    total = part_ref[0]
    for n in range(1, part_ref.shape[0]):
        total = total + part_ref[n]
    total = total * factor
    nmom = out_ref.shape[2]
    for k in range(out_ref.shape[0]):
        for c in range(2):
            first = (k // 4) * 64 + c * 32
            moved = total if first == 0 else pltpu.roll(total, LANES - first, 1)
            out_ref[k, c : c + 1, :] = moved[k % 4 : k % 4 + 1, 0:nmom]


def summed_traces(parts, factor, npairs, nmom):
    return pl.pallas_call(
        functools.partial(correlators_kernel, factor),
        out_shape=jax.ShapeDtypeStruct((npairs, 2, nmom), jnp.float32),
        compiler_params=grant(4),
        name="correlators",
    )(parts)


def exchange(array, axis):
    return lax.all_to_all(array, axis, split_axis=0, concat_axis=0, tiled=True)


def local(solutions, noise, momenta, pairs):
    spincol, sites, width = solutions.shape[1:]
    nmom = momenta.shape[0]
    peer, own = partial_fields(momenta.T, jnp.swapaxes(noise[0], 0, 1), solutions[0])
    arrived = lax.ppermute(peer, "core", [(0, 1), (1, 0)])
    scale = 1.0 / math.sqrt(spincol * sites * 2 * ZY)
    copies, mesons = summed_mesons(exchange((own + arrived).reshape(ZY, BLOCK, LANES), ("z", "yh")), scale, lax.axis_size("tm"), nmom)
    traces, mesons = partial_traces(pairs.T, mesons, exchange(copies, "tm"))
    traces = traces + lax.ppermute(traces, "core", [(0, 1), (1, 0)])
    spread = jnp.broadcast_to(traces, (ZY, *traces.shape))
    correlators = summed_traces(exchange(spread, ("yh", "z")), 1.0 / 64, pairs.shape[0], nmom)
    return (mesons, correlators)


def solution(mesh):
    split = Mesh(mesh.devices.reshape(8, 2, 2, 8), ("z", "yh", "core", "tm"))
    space = ("z", "yh", "core")
    in_specs = (P("tm", None, space, None), P("tm", None, None, space), P(), P("tm", None))
    out_specs = (P("tm", None, None, space, None), P("tm", None, None))
    return jax.shard_map(local, mesh=split, in_specs=in_specs, out_specs=out_specs, check_vma=False)
```
